32 devices in a mesh: rep: 1 (over z), data: 4 (over y), expert: 8 (over x, core).
Axes of the slice: x: 4, y: 4, z: 1, core: 2. Of those that a mesh axis runs over, the one named last changes fastest.
The devices are a block of a 4x4x8 slice.
Arguments:
- x_in: bfloat16 [2, 16384, 2048], P(None, ('rep', 'expert', 'data'))
- expert_idx: int32 [2, 16384, 6], P(None, ('rep', 'expert', 'data'))
- gate_wt: float32 [2, 16384, 6], P(None, ('rep', 'expert', 'data'))
- w_gate: bfloat16 [64, 2048, 1408], P('expert', 'data')
- w_up: bfloat16 [64, 2048, 1408], P('expert', 'data')
- w_down: bfloat16 [64, 1408, 2048], P('expert', None, 'data')
Outputs:
- output: bfloat16 [2, 16384, 2048], P(None, ('rep', 'expert', 'data'))
All inputs are finite; a program needn't handle non-finite values.
Results may differ from the reference program's by a relative error of at most 0.00131.
Values are sent between devices in bfloat16 or wider.
A program may use at most 768 MiB of HBM per device.

```python
import jax
import jax.numpy as jnp
from jax import lax

D_MODEL = 2048
FF = 1408
N_EXP = 64
TOP = 6
TOK_LOC = 512
EXPERT_DEVS = 8
DATA_DEVS = 4
CAP = 64


def draw_routing(route_key):
    dev_count = EXPERT_DEVS * DATA_DEVS
    key_noise, key_bias, key_hot, key_perm = jax.random.split(route_key, 4)
    draw_noise = jax.random.randint(key_noise, (2, dev_count, TOK_LOC, N_EXP), 0, 4096)
    exp_bias = jax.random.randint(key_bias, (2, 1, 1, N_EXP), 0, 1024)
    hot_id = jax.random.randint(key_hot, (2, dev_count, 1, 1), 0, N_EXP)
    perm_keys = jax.random.split(key_perm, 2 * dev_count)
    tok_rank = jax.vmap(lambda sub_key: jax.random.permutation(sub_key, TOK_LOC))(perm_keys)
    tok_rank = tok_rank.reshape(2, dev_count, TOK_LOC, 1)
    hot_count = min(TOK_LOC, CAP + CAP // 4)
    expert_ids = jnp.arange(N_EXP, dtype=jnp.int32)
    forced = jnp.logical_and(tok_rank < hot_count, expert_ids == hot_id).astype(jnp.int32)
    int_score = (draw_noise + exp_bias + forced * 8192) * N_EXP + expert_ids
    chosen = lax.top_k(int_score, TOP)[1].astype(jnp.int32)
    return chosen.reshape(2, dev_count * TOK_LOC, TOP)


def setup_inputs(seed: int = 0, part: int = 0) -> dict:
    base_key = jax.random.key(seed)
    shared_key, token_key = jax.random.split(base_key)
    part_key = jax.random.fold_in(token_key, part)
    key_x, key_route, key_gate = jax.random.split(part_key, 3)
    key_wg, key_wu, key_wd = jax.random.split(shared_key, 3)
    tok_all = EXPERT_DEVS * DATA_DEVS * TOK_LOC
    x_in = jax.random.normal(key_x, (2, tok_all, D_MODEL), jnp.float32).astype(jnp.bfloat16)
    expert_idx = draw_routing(key_route)
    gate_wt = jax.random.uniform(key_gate, (2, tok_all, TOP), jnp.float32, 0.2, 0.8)
    w_gate = (jax.random.normal(key_wg, (N_EXP, D_MODEL, FF), jnp.float32) * D_MODEL ** -0.5).astype(jnp.bfloat16)
    w_up = (jax.random.normal(key_wu, (N_EXP, D_MODEL, FF), jnp.float32) * D_MODEL ** -0.5).astype(jnp.bfloat16)
    w_down = (jax.random.normal(key_wd, (N_EXP, FF, D_MODEL), jnp.float32) * (1.5 * FF ** -0.5)).astype(jnp.bfloat16)
    return {'x_in': x_in, 'expert_idx': expert_idx, 'gate_wt': gate_wt, 'w_gate': w_gate, 'w_up': w_up, 'w_down': w_down}


def slot_table(ids_block):
    flat_ids = ids_block.reshape(-1)
    one_hot = (flat_ids[:, None] == jnp.arange(N_EXP, dtype=jnp.int32)[None, :]).astype(jnp.int32)
    slot_of = jnp.sum((jnp.cumsum(one_hot, axis=0) - one_hot) * one_hot, axis=1)
    return flat_ids, slot_of


def expert_ffn(rows_in, wg_one, wu_one, wd_one):
    gate_pre = jnp.dot(rows_in, wg_one, preferred_element_type=jnp.float32)
    up_pre = jnp.dot(rows_in, wu_one, preferred_element_type=jnp.float32)
    hidden = (jax.nn.silu(gate_pre) * up_pre).astype(jnp.bfloat16)
    return jnp.dot(hidden, wd_one, preferred_element_type=jnp.float32).astype(jnp.bfloat16)


def moe_micro(x_mb, idx_mb, gate_mb, w_gate, w_up, w_down):
    dev_count = EXPERT_DEVS * DATA_DEVS
    pair_count = TOK_LOC * TOP
    slot_total = N_EXP * CAP
    x_blocks = x_mb.reshape(dev_count, TOK_LOC, D_MODEL)
    flat_ids, slot_of = jax.vmap(slot_table)(idx_mb.reshape(dev_count, TOK_LOC, TOP))
    is_kept = slot_of < CAP
    dest_pos = jnp.where(is_kept, flat_ids * CAP + slot_of, slot_total)
    pair_ids = jnp.arange(pair_count, dtype=jnp.int32)
    source_of = jax.vmap(lambda dest_row: jnp.full((slot_total,), pair_count, jnp.int32).at[dest_row].set(pair_ids, mode='drop'))(dest_pos)
    tok_of = jnp.minimum(source_of // TOP, TOK_LOC - 1)
    buffers = jax.vmap(lambda x_blk, tok_row: x_blk[tok_row])(x_blocks, tok_of)
    buffers = jnp.where((source_of < pair_count)[:, :, None], buffers, jnp.zeros((), jnp.bfloat16))
    per_expert = buffers.reshape(dev_count, N_EXP, CAP, D_MODEL).transpose(1, 0, 2, 3).reshape(N_EXP, dev_count * CAP, D_MODEL)
    expert_out = lax.map(lambda expert_args: expert_ffn(expert_args[0], expert_args[1], expert_args[2], expert_args[3]), (per_expert, w_gate, w_up, w_down))
    back_rows = expert_out.reshape(N_EXP, dev_count, CAP, D_MODEL).transpose(1, 0, 2, 3).reshape(dev_count, slot_total, D_MODEL)
    pair_out = jax.vmap(lambda back_blk, pos_row: back_blk[pos_row])(back_rows, jnp.minimum(dest_pos, slot_total - 1))
    pair_out = pair_out.reshape(dev_count, TOK_LOC, TOP, D_MODEL).astype(jnp.float32)
    weight = jnp.where(is_kept.reshape(dev_count, TOK_LOC, TOP), gate_mb.reshape(dev_count, TOK_LOC, TOP), 0.0)
    mix_sum = jnp.sum(pair_out * weight[:, :, :, None], axis=2)
    y_blocks = (x_blocks.astype(jnp.float32) + mix_sum).astype(jnp.bfloat16)
    return y_blocks.reshape(dev_count * TOK_LOC, D_MODEL)


def reference(x_in, expert_idx, gate_wt, w_gate, w_up, w_down):
    return lax.map(lambda mb_args: moe_micro(mb_args[0], mb_args[1], mb_args[2], w_gate, w_up, w_down), (x_in, expert_idx, gate_wt))
```

```python
import functools

import jax
import jax.numpy as jnp
from jax import lax
from jax.experimental import pallas as pl
from jax.experimental.pallas import tpu as pltpu
from jax.sharding import PartitionSpec as P

MESH = pl.DeviceIdType.MESH
LANES = 128


def moe_kernel(n_x, cap, x_ref, ids_ref, gate_ref, wg_ref, wu_ref, wd_ref,
               y_ref, xg_ref, rb_ref, bk_ref, lg_ref, lu_ref, ld_ref,
               wg_v, wu_v, wd_v, rows_v, o_v, h_v, acc_v, send_v, ob_v, lt_v, p_v, g_v, pl_v,
               ws, wr, wl, xs, xr, ps, pr, xsem, ssem, rsem, bs, b0, br, br0, osem, ysem):
    n_mb, n_blk, _, d_model = x_ref.shape
    tok = n_blk * cap
    n_loc, d_loc, ff = wg_ref.shape
    half = n_loc // 2
    n_quad = n_blk * 2
    n_exp = n_blk * n_loc
    n_top = ids_ref.shape[1]
    n_tile = 256

    e = lax.axis_index('expert')
    d = lax.axis_index('data')
    x = e // 2
    c = e % 2
    h = d // 2
    twin_d = d + 1 - 2 * (d % 2)
    part_d = 3 - d

    def dev(line, r, cc):
        return {'expert': 2 * ((x + r) % n_x) + (c + cc) % 2, 'data': d + line * (part_d - d)}

    def quad(line, rc):
        r, cc = rc // 2, rc % 2
        return 2 * (2 * ((x + r) % n_x) + (c + cc) % 2) + (h + line * (1 - 2 * h))

    twin = {'expert': e, 'data': twin_d}
    partner = {'expert': e, 'data': part_d}
    self_q = quad(0, 0)

    peers = [dev(line, r, cc) for line in range(2) for r in range(n_x) for cc in range(2) if (line, r, cc) != (0, 0, 0)]
    barrier = pltpu.get_barrier_semaphore()
    for peer in peers + [twin]:
        pl.semaphore_signal(barrier, inc=1, device_id=peer, device_id_type=MESH)
    pl.semaphore_wait(barrier, len(peers) + 1)

    def remote(src, dst, send_sem, recv_sem, device):
        return pltpu.make_async_remote_copy(src_ref=src, dst_ref=dst, send_sem=send_sem, recv_sem=recv_sem,
                                            device_id=device, device_id_type=MESH)

    w_in = (wg_ref, wu_ref, wd_ref)
    w_land = (lg_ref, lu_ref, ld_ref)

    def w_copy(flow, k, a):
        if flow == 0:
            src, device = w_in[a].at[half * h + k], twin
        elif flow == 1:
            src, device = w_in[a].at[half * (1 - h) + k], partner
        else:
            src, device = w_land[a].at[1, k], twin
        return remote(src, w_land[a].at[flow, k], ws.at[flow, k, a], wr.at[flow, k, a], device)

    def w_start(flow, k):
        for a in range(3):
            w_copy(flow, k, a).start()

    def w_forward(k):
        for a in range(3):
            w_copy(1, k, a).wait_recv()
            w_copy(2, k, a).start()

    def x_slot(line, mb, r, cc):
        return xg_ref.at[mb, line * n_blk + r * 2 + cc]

    def x_have(line, mb, r):
        return x_ref.at[mb] if (line, r) == (0, 0) else x_slot(line, mb, r, 0)

    def x_copy(line, mb, r, cc):
        if cc == 1:
            src, device = x_have(line, mb, r), dev(0, 0, 1)
        elif r == 0:
            src, device = x_ref.at[mb], partner
        elif r == n_x - 1:
            src, device = x_have(line, mb, 0), dev(0, 1, 0)
        elif r == 1:
            src, device = x_have(line, mb, 0), dev(0, n_x - 1, 0)
        elif mb == 0:
            src, device = x_have(line, mb, n_x - 1), dev(0, 1, 0)
        else:
            src, device = x_have(line, mb, 1), dev(0, n_x - 1, 0)
        i = line * n_blk + r * 2 + cc
        return remote(src, x_slot(line, mb, r, cc), xs.at[mb, i], xr.at[mb, i], device)

    def x_start(*keys):
        for key in keys:
            x_copy(*key).start()

    def x_wait(*key):
        x_copy(*key).wait_recv()

    def p_copy(line, r, cc):
        rr = (n_x - r) % n_x
        i = line * n_blk + rr * 2 + cc
        return remote(p_v.at[quad(line, r * 2 + cc)], pl_v.at[i], ps.at[i], pr.at[i], dev(line, r, cc))

    w_start(0, 0)
    for mb in range(n_mb):
        x_start((1, mb, 0, 0), (0, mb, 3, 0), (0, mb, 1, 0), (0, mb, 0, 1))

    row_i = lax.broadcasted_iota(jnp.int32, (tok, tok), 0)
    col_i = lax.broadcasted_iota(jnp.int32, (tok, tok), 1)
    earlier = jnp.where(row_i < col_i, 1.0, 0.0).astype(jnp.bfloat16)
    exp_i = lax.broadcasted_iota(jnp.int32, (n_exp, tok), 0)
    for mb in range(n_mb):
        picked = jnp.zeros((n_exp, tok), jnp.float32)
        weight = jnp.zeros((n_exp, tok), jnp.float32)
        for j in range(n_top):
            match = exp_i == ids_ref[mb, j:j + 1, :]
            picked = picked + jnp.where(match, 1.0, 0.0)
            weight = weight + jnp.where(match, gate_ref[mb, j:j + 1, :], 0.0)
        place = jnp.dot(picked.astype(jnp.bfloat16), earlier, preferred_element_type=jnp.float32)
        slot_of = jnp.where(picked > 0.5, jnp.where(place < cap - 0.5, place, -1.0), -1.0)
        p_v[:, mb * half:(mb + 1) * half, :] = slot_of.reshape(n_quad, half, tok)
        g_v[:, mb * half:(mb + 1) * half, :] = weight.reshape(n_quad, half, tok)
    for line in range(2):
        for r in range(n_x):
            for cc in range(2):
                if (line, r, cc) != (0, 0, 0):
                    p_copy(line, r, cc).start()
    w_start(0, 1)
    for k in range(half):
        w_start(1, k)
    pl_v[0] = p_v[self_q]

    for mb in range(n_mb):
        pltpu.make_async_copy(x_ref.at[mb], rows_v.at[mb], xsem.at[mb]).start()
    for mb in range(n_mb):
        pltpu.make_async_copy(x_ref.at[mb], rows_v.at[mb], xsem.at[mb]).wait()
        pltpu.make_async_copy(rows_v.at[mb], x_slot(0, mb, 0, 0), xsem.at[mb]).start()
        acc_v[mb] = rows_v[mb].reshape(tok, d_model).astype(jnp.float32)

    x_wait(0, 0, 3, 0)
    x_start((0, 0, 2, 0), (0, 0, 3, 1))
    x_wait(0, 0, 1, 0)
    x_start((0, 0, 1, 1))
    x_wait(1, 0, 0, 0)
    x_start((1, 0, 3, 0), (1, 0, 1, 0), (1, 0, 0, 1))
    x_wait(0, 1, 3, 0)
    x_start((0, 1, 3, 1))
    x_wait(0, 1, 1, 0)
    x_start((0, 1, 2, 0), (0, 1, 1, 1))
    x_wait(1, 1, 0, 0)
    x_start((1, 1, 3, 0), (1, 1, 1, 0), (1, 1, 0, 1))
    x_wait(0, 0, 2, 0)
    x_start((0, 0, 2, 1))
    x_wait(1, 0, 1, 0)
    x_start((1, 0, 1, 1))
    x_wait(1, 0, 3, 0)
    x_start((1, 0, 2, 0), (1, 0, 3, 1))
    x_wait(0, 1, 2, 0)
    x_start((0, 1, 2, 1))
    w_forward(0)
    w_start(0, 2)
    x_wait(1, 1, 3, 0)
    x_start((1, 1, 3, 1))
    x_wait(1, 1, 1, 0)
    x_start((1, 1, 2, 0), (1, 1, 1, 1))
    x_wait(1, 0, 2, 0)
    x_start((1, 0, 2, 1))
    x_wait(1, 1, 2, 0)
    x_start((1, 1, 2, 1))
    w_forward(1)
    w_start(0, 3)
    for line in range(2):
        for mb in range(n_mb):
            for r in range(n_x):
                x_wait(line, mb, r, 1)
    for line in range(2):
        for r in range(n_x):
            for cc in range(2):
                if (line, r, cc) != (0, 0, 0):
                    p_copy(line, (n_x - r) % n_x, cc).wait_recv()
    for mb in range(n_mb):
        pltpu.make_async_copy(rows_v.at[mb], x_slot(0, mb, 0, 0), xsem.at[mb]).wait()

    n_unit = n_mb * 2 * n_blk
    place_i = lax.broadcasted_iota(jnp.int32, (cap, tok), 0).astype(jnp.float32)

    def x_load(u):
        slot = u % 2
        return pltpu.make_async_copy(xg_ref.at[u // (2 * n_blk), u % (2 * n_blk)], rows_v.at[slot], xsem.at[slot])

    def row_store(u):
        slot = u % 2
        mb, i = u // (2 * n_blk), u % (2 * n_blk)
        return pltpu.make_async_copy(send_v.at[slot], rb_ref.at[pl.ds(0, half), mb, i // n_blk, i % n_blk], ssem.at[slot])

    x_load(0).start()

    def dispatch(u, carry):
        slot = u % 2
        mb, i = u // (2 * n_blk), u % (2 * n_blk)
        x_load(u).wait()

        @pl.when(u + 1 < n_unit)
        def _():
            x_load(u + 1).start()

        pick = jnp.concatenate(
            [jnp.where(pl_v[i, pl.ds(mb * half + k, 1), :] == place_i, 1.0, 0.0) for k in range(half)], axis=0)
        pick = pick.astype(jnp.bfloat16)

        @pl.when(u >= 2)
        def _():
            row_store(u - 2).wait()

        def tile(n, carry):
            cols = pl.ds(pl.multiple_of(n * n_tile, n_tile), n_tile)
            block = rows_v[slot, :, :, cols].reshape(tok, n_tile)
            got = jnp.dot(pick, block, preferred_element_type=jnp.float32).astype(jnp.bfloat16)
            send_v[slot, :, :, cols] = got.reshape(half, cap, n_tile)
            return carry

        lax.fori_loop(0, d_model // n_tile, tile, 0)
        row_store(u).start()
        return carry

    lax.fori_loop(0, n_unit, dispatch, 0)
    row_store(n_unit - 2).wait()
    row_store(n_unit - 1).wait()

    n_chunk = 2 * n_mb
    rows_chunk = n_blk * cap

    def chunk_of(ck):
        return 1 - ck // n_mb, ck % n_mb

    def row_load(k, ck):
        line, mb = chunk_of(ck)
        return pltpu.make_async_copy(rb_ref.at[k, mb, line], rows_v.at[ck % 2], rsem.at[ck % 2])

    def w_load(j, k, a):
        owner = (twin_d, part_d, 3 - twin_d, d)[j]
        at = pl.ds(pl.multiple_of(owner * d_loc, d_loc), d_loc)
        src = w_in[a].at[half * h + k] if j == 3 else w_land[a].at[j, k]
        dst = wd_v.at[:, at] if a == 2 else (wg_v, wu_v)[a].at[at, :]
        return pltpu.make_async_copy(src, dst, wl.at[j, a])

    def far_send(k, ck, rc):
        line, mb = chunk_of(ck)
        r, cc = rc // 2, rc % 2
        back = ((n_x - r) % n_x) * 2 + cc
        return remote(o_v.at[ck, rc], bk_ref.at[k, mb, line, back], bs.at[ck], br.at[k, ck], dev(line, r, cc))

    def near_send(k, ck):
        line, mb = chunk_of(ck)
        return remote(o_v.at[ck, 0], bk_ref.at[k, mb, line, 0], b0.at[ck], br0.at[k, mb], partner)

    def near_copy(k, ck):
        line, mb = chunk_of(ck)
        return pltpu.make_async_copy(o_v.at[ck, 0], bk_ref.at[k, mb, line, 0], b0.at[ck])

    def sent_wait(ck):
        many = o_v.at[ck, pl.ds(1, n_blk - 1)]
        pltpu.make_async_copy(many, many, bs.at[ck]).wait()
        one = o_v.at[ck, 0]
        pltpu.make_async_copy(one, one, b0.at[ck]).wait()

    def compute(k):
        row_load(k, 0).start()
        for a in range(3):
            w_load(3, k, a).start()
        for j in range(3):
            for a in range(3):
                if j != 1:
                    w_copy(j, k, a).wait_recv()
                w_load(j, k, a).start()
        for j in range(4):
            for a in range(3):
                w_load(j, k, a).wait()

        def chunk(ck, carry):
            slot = ck % 2
            row_load(k, ck).wait()

            @pl.when(ck + 1 < n_chunk)
            def _():
                row_load(k, ck + 1).start()

            def up_tile(f, carry):
                cols = pl.ds(pl.multiple_of(f * LANES, LANES), LANES)
                both = jnp.concatenate([wg_v[:, cols], wu_v[:, cols]], axis=1)
                pre = jnp.dot(rows_v[slot].reshape(rows_chunk, d_model), both, preferred_element_type=jnp.float32)
                h_v[:, cols] = (jax.nn.silu(pre[:, :LANES]) * pre[:, LANES:]).astype(jnp.bfloat16)
                return carry

            lax.fori_loop(0, ff // LANES, up_tile, 0)

            @pl.when(k > 0)
            def _():
                sent_wait(ck)

            def down_tile(n, carry):
                cols = pl.ds(pl.multiple_of(n * n_tile, n_tile), n_tile)
                out = jnp.dot(h_v[...], wd_v[:, cols], preferred_element_type=jnp.float32).astype(jnp.bfloat16)
                o_v[ck, :, :, cols] = out.reshape(n_blk, cap, n_tile)
                return carry

            lax.fori_loop(0, d_model // n_tile, down_tile, 0)

            for rc in range(1, n_blk):
                far_send(k, ck, rc).start()

            @pl.when(ck < n_mb)
            def _():
                near_send(k, ck).start()

            @pl.when(ck >= n_mb)
            def _():
                near_copy(k, ck).start()

            return carry

        lax.fori_loop(0, n_chunk, chunk, 0)

    n_grp = n_blk // 4
    k_rows = 4 * cap

    def o_load(k, u):
        line, mb = chunk_of(u // n_grp)
        return pltpu.make_async_copy(bk_ref.at[k, mb, line, pl.ds((u % n_grp) * 4, 4)], ob_v.at[u % 2], osem.at[u % 2])

    def o_ready(k, u):
        ck = u // n_grp
        line, mb = chunk_of(ck)

        @pl.when(u % n_grp == 0)
        def _():
            many = bk_ref.at[k, mb, line, pl.ds(1, n_blk - 1)]
            pltpu.make_async_copy(many, many, br.at[k, ck]).wait()

        @pl.when(jnp.logical_and(u % n_grp == 0, ck < n_mb))
        def _():
            near_send(k, ck).wait_recv()

        o_load(k, u).start()

    def combine(k):
        o_ready(k, 0)

        def unit(u, carry):
            line, mb = chunk_of(u // n_grp)
            slot = u % 2
            parts = []
            for i in range(4):
                q = quad(line, (u % n_grp) * 4 + i)
                hit = p_v[q, pl.ds(mb * half + k, 1), :] == place_i
                parts.append(jnp.where(hit, g_v[q, pl.ds(mb * half + k, 1), :], 0.0))
            mix = jnp.concatenate(parts, axis=0).T
            first = mix.astype(jnp.bfloat16)
            rest = mix - first.astype(jnp.float32)
            second = rest.astype(jnp.bfloat16)
            third = (rest - second.astype(jnp.float32)).astype(jnp.bfloat16)
            lt_v[:, 0:k_rows] = first
            lt_v[:, k_rows:2 * k_rows] = second
            lt_v[:, 2 * k_rows:3 * k_rows] = third
            o_load(k, u).wait()

            @pl.when(u + 1 < n_chunk * n_grp)
            def _():
                o_ready(k, u + 1)

            def tile(n, carry):
                cols = pl.ds(pl.multiple_of(n * n_tile, n_tile), n_tile)
                rows = ob_v[slot, :, :, cols].reshape(k_rows, n_tile)
                acc_v[mb, :, cols] += jnp.dot(lt_v[...], jnp.concatenate([rows, rows, rows], axis=0),
                                              preferred_element_type=jnp.float32)
                return carry

            lax.fori_loop(0, d_model // n_tile, tile, 0)
            return carry

        lax.fori_loop(0, n_chunk * n_grp, unit, 0)

    def step(k, carry):
        @pl.when(k < half)
        def _():
            compute(k)

        @pl.when(k + 2 < half)
        def _():
            w_forward(k + 2)

        @pl.when(k == half)
        def _():
            for ck in range(n_chunk):
                sent_wait(ck)

        @pl.when(k > 0)
        def _():
            combine(k - 1)

        return carry

    lax.fori_loop(0, half + 1, step, 0)

    for mb in range(n_mb):
        rows_v[mb] = acc_v[mb].astype(jnp.bfloat16).reshape(n_blk, cap, d_model)
        pltpu.make_async_copy(rows_v.at[mb], y_ref.at[mb], ysem.at[mb]).start()

    for flow in range(3):
        for k in range(half):
            for a in range(3):
                w_copy(flow, k, a).wait_send()
    for line in range(2):
        for mb in range(n_mb):
            for r in range(n_x):
                for cc in range(2):
                    if (line, r, cc) != (0, 0, 0):
                        x_copy(line, mb, r, cc).wait_send()
    for line in range(2):
        for r in range(n_x):
            for cc in range(2):
                if (line, r, cc) != (0, 0, 0):
                    p_copy(line, r, cc).wait_send()
    for mb in range(n_mb):
        pltpu.make_async_copy(rows_v.at[mb], y_ref.at[mb], ysem.at[mb]).wait()


def solution(mesh):
    expert_devs = mesh.shape['expert']
    n_x = expert_devs // 2
    row_spec = P(None, ('rep', 'expert', 'data'), None)
    up_spec = P('expert', 'data', None)
    down_spec = P('expert', None, 'data')

    def per_device(x_loc, idx_loc, gate_loc, wg_loc, wu_loc, wd_loc):
        n_mb, tok, d_model = x_loc.shape
        n_top = idx_loc.shape[2]
        n_loc, d_loc, ff = wg_loc.shape
        n_exp = n_loc * expert_devs
        half = n_loc // 2
        cap = 8 * ((5 * n_top * tok + 32 * n_exp - 1) // (32 * n_exp))
        assert tok == expert_devs * cap
        bf16, f32 = jnp.bfloat16, jnp.float32
        n_quad = 2 * expert_devs
        rows = (expert_devs, cap, d_model)
        hbm = pl.BlockSpec(memory_space=pl.ANY)
        vmem = pl.BlockSpec(memory_space=pltpu.VMEM)
        dma = pltpu.SemaphoreType.DMA
        out = pl.pallas_call(
            functools.partial(moe_kernel, n_x, cap),
            out_shape=[
                jax.ShapeDtypeStruct((n_mb,) + rows, bf16),
                jax.ShapeDtypeStruct((n_mb, n_quad) + rows, bf16),
                jax.ShapeDtypeStruct((half, n_mb, 2) + rows, bf16),
                jax.ShapeDtypeStruct((half, n_mb, 2) + rows, bf16),
                jax.ShapeDtypeStruct((3, half, d_loc, ff), bf16),
                jax.ShapeDtypeStruct((3, half, d_loc, ff), bf16),
                jax.ShapeDtypeStruct((3, half, ff, d_loc), bf16),
            ],
            in_specs=[hbm, vmem, vmem, hbm, hbm, hbm],
            out_specs=[hbm] * 7,
            scratch_shapes=[
                pltpu.VMEM((4 * d_loc, ff), bf16),
                pltpu.VMEM((4 * d_loc, ff), bf16),
                pltpu.VMEM((ff, 4 * d_loc), bf16),
                pltpu.VMEM((2,) + rows, bf16),
                pltpu.VMEM((2 * n_mb,) + rows, bf16),
                pltpu.VMEM((tok, ff), bf16),
                pltpu.VMEM((n_mb, tok, d_model), f32),
                pltpu.VMEM((2, half, cap, d_model), bf16),
                pltpu.VMEM((2, 4, cap, d_model), bf16),
                pltpu.VMEM((tok, 12 * cap), bf16),
                pltpu.VMEM((n_quad, n_mb * half, tok), f32),
                pltpu.VMEM((n_quad, n_mb * half, tok), f32),
                pltpu.VMEM((n_quad, n_mb * half, tok), f32),
                dma((3, half, 3)), dma((3, half, 3)), dma((4, 3)),
                dma((n_mb, n_quad)), dma((n_mb, n_quad)),
                dma((n_quad,)), dma((n_quad,)),
                dma((2,)), dma((2,)), dma((2,)),
                dma((2 * n_mb,)), dma((2 * n_mb,)),
                dma((half, 2 * n_mb)), dma((half, n_mb)),
                dma((2,)), dma((2,)),
            ],
            compiler_params=pltpu.CompilerParams(collective_id=0, has_side_effects=True, vmem_limit_bytes=62 * 1024 * 1024),
        )(x_loc.reshape((n_mb,) + rows), idx_loc.transpose(0, 2, 1), gate_loc.transpose(0, 2, 1), wg_loc, wu_loc, wd_loc)
        return out[0].reshape(n_mb, tok, d_model)

    return jax.shard_map(per_device, mesh=mesh, in_specs=(row_spec, row_spec, row_spec, up_spec, up_spec, down_spec),
                         out_specs=row_spec, check_vma=False)
```

```python
import functools

import jax
import jax.numpy as jnp
from jax import lax
from jax.experimental import pallas as pl
from jax.experimental.pallas import tpu as pltpu
from jax.sharding import PartitionSpec as P

MESH = pl.DeviceIdType.MESH
LANES = 128


def moe_kernel(n_x, cap, x_ref, ids_ref, gate_ref, wg_ref, wu_ref, wd_ref,
               y_ref, xg_ref, rb_ref, bk_ref, lg_ref, lu_ref, ld_ref,
               wg_v, wu_v, wd_v, rows_v, o_v, h_v, acc_v, send_v, ob_v, lt_v, p_v, g_v, pl_v,
               ws, wr, wl, xs, xr, ps, pr, xsem, ssem, rsem, bs, b0, br, br0, osem, ysem):
    n_mb, n_blk, _, d_model = x_ref.shape
    tok = n_blk * cap
    n_loc, d_loc, ff = wg_ref.shape
    half = n_loc // 2
    n_quad = n_blk * 2
    n_exp = n_blk * n_loc
    n_top = ids_ref.shape[0]
    n_tile = 256

    e = lax.axis_index('expert')
    d = lax.axis_index('data')
    x = e // 2
    c = e % 2
    h = d // 2
    twin_d = d + 1 - 2 * (d % 2)
    part_d = 3 - d

    def dev(line, r, cc):
        return {'expert': 2 * ((x + r) % n_x) + (c + cc) % 2, 'data': d + line * (part_d - d)}

    def quad(line, rc):
        r, cc = rc // 2, rc % 2
        return 2 * (2 * ((x + r) % n_x) + (c + cc) % 2) + (h + line * (1 - 2 * h))

    twin = {'expert': e, 'data': twin_d}
    partner = {'expert': e, 'data': part_d}
    self_q = quad(0, 0)

    peers = [dev(line, r, cc) for line in range(2) for r in range(n_x) for cc in range(2) if (line, r, cc) != (0, 0, 0)]
    barrier = pltpu.get_barrier_semaphore()
    for peer in peers + [twin]:
        pl.semaphore_signal(barrier, inc=1, device_id=peer, device_id_type=MESH)
    pl.semaphore_wait(barrier, len(peers) + 1)

    def remote(src, dst, send_sem, recv_sem, device):
        return pltpu.make_async_remote_copy(src_ref=src, dst_ref=dst, send_sem=send_sem, recv_sem=recv_sem,
                                            device_id=device, device_id_type=MESH)

    w_in = (wg_ref, wu_ref, wd_ref)
    w_land = (lg_ref, lu_ref, ld_ref)

    def w_copy(flow, k, a):
        if flow == 0:
            src, device = w_in[a].at[half * h + k], twin
        elif flow == 1:
            src, device = w_in[a].at[half * (1 - h) + k], partner
        else:
            src, device = w_land[a].at[1, k], twin
        return remote(src, w_land[a].at[flow, k], ws.at[flow, k, a], wr.at[flow, k, a], device)

    def w_start(flow, k):
        for a in range(3):
            w_copy(flow, k, a).start()

    def w_forward(k):
        for a in range(3):
            w_copy(1, k, a).wait_recv()
            w_copy(2, k, a).start()

    def x_slot(line, mb, r, cc):
        return xg_ref.at[mb, line * n_blk + r * 2 + cc]

    def x_have(line, mb, r):
        return x_ref.at[mb] if (line, r) == (0, 0) else x_slot(line, mb, r, 0)

    def x_copy(line, mb, r, cc):
        if cc == 1:
            src, device = x_have(line, mb, r), dev(0, 0, 1)
        elif r == 0:
            src, device = x_ref.at[mb], partner
        elif r == n_x - 1:
            src, device = x_have(line, mb, 0), dev(0, 1, 0)
        elif r == 1:
            src, device = x_have(line, mb, 0), dev(0, n_x - 1, 0)
        elif mb == 0:
            src, device = x_have(line, mb, n_x - 1), dev(0, 1, 0)
        else:
            src, device = x_have(line, mb, 1), dev(0, n_x - 1, 0)
        i = line * n_blk + r * 2 + cc
        return remote(src, x_slot(line, mb, r, cc), xs.at[mb, i], xr.at[mb, i], device)

    def x_start(*keys):
        for key in keys:
            x_copy(*key).start()

    def x_wait(*key):
        with jax.named_scope('x%d%d%d%d' % key):
            x_copy(*key).wait_recv()

    def p_copy(line, r, cc):
        rr = (n_x - r) % n_x
        i = line * n_blk + rr * 2 + cc
        return remote(p_v.at[quad(line, r * 2 + cc)], pl_v.at[i], ps.at[i], pr.at[i], dev(line, r, cc))

    w_start(0, 0)
    for mb in range(n_mb):
        x_start((1, mb, 0, 0), (0, mb, 3, 0), (0, mb, 1, 0), (0, mb, 0, 1))

    row_i = lax.broadcasted_iota(jnp.int32, (tok, tok), 0)
    col_i = lax.broadcasted_iota(jnp.int32, (tok, tok), 1)
    earlier = jnp.where(row_i < col_i, 1.0, 0.0).astype(jnp.bfloat16)
    exp_i = lax.broadcasted_iota(jnp.int32, (n_exp, tok), 0)
    for mb in range(n_mb):
        picked = jnp.zeros((n_exp, tok), jnp.float32)
        weight = jnp.zeros((n_exp, tok), jnp.float32)
        for j in range(n_top):
            match = exp_i == ids_ref[j, mb:mb + 1, :]
            picked = picked + jnp.where(match, 1.0, 0.0)
            weight = weight + jnp.where(match, gate_ref[j, mb:mb + 1, :], 0.0)
        place = jnp.dot(picked.astype(jnp.bfloat16), earlier, preferred_element_type=jnp.float32)
        slot_of = jnp.where(picked > 0.5, jnp.where(place < cap - 0.5, place, -1.0), -1.0)
        p_v[:, mb * half:(mb + 1) * half, :] = slot_of.reshape(n_quad, half, tok)
        g_v[:, mb * half:(mb + 1) * half, :] = weight.reshape(n_quad, half, tok)
    for line in range(2):
        for r in range(n_x):
            for cc in range(2):
                if (line, r, cc) != (0, 0, 0):
                    p_copy(line, r, cc).start()
    w_start(0, 1)
    for k in range(half):
        w_start(1, k)
    pl_v[0] = p_v[self_q]

    for mb in range(n_mb):
        pltpu.make_async_copy(x_ref.at[mb], rows_v.at[mb], xsem.at[mb]).start()
    for mb in range(n_mb):
        pltpu.make_async_copy(x_ref.at[mb], rows_v.at[mb], xsem.at[mb]).wait()
        pltpu.make_async_copy(rows_v.at[mb], x_slot(0, mb, 0, 0), xsem.at[mb]).start()
        acc_v[mb] = rows_v[mb].reshape(tok, d_model).astype(jnp.float32)

    x_wait(0, 0, 3, 0)
    x_start((0, 0, 2, 0), (0, 0, 3, 1))
    x_wait(0, 0, 1, 0)
    x_start((0, 0, 1, 1))
    x_wait(1, 0, 0, 0)
    x_start((1, 0, 3, 0), (1, 0, 1, 0), (1, 0, 0, 1))
    x_wait(0, 1, 3, 0)
    x_start((0, 1, 3, 1))
    x_wait(0, 1, 1, 0)
    x_start((0, 1, 2, 0), (0, 1, 1, 1))
    x_wait(1, 1, 0, 0)
    x_start((1, 1, 3, 0), (1, 1, 1, 0), (1, 1, 0, 1))
    x_wait(0, 0, 2, 0)
    x_start((0, 0, 2, 1))
    x_wait(1, 0, 1, 0)
    x_start((1, 0, 1, 1))
    x_wait(1, 0, 3, 0)
    x_start((1, 0, 2, 0), (1, 0, 3, 1))
    x_wait(0, 1, 2, 0)
    x_start((0, 1, 2, 1))
    with jax.named_scope('fwd0'):
        w_forward(0)
    x_wait(1, 1, 3, 0)
    x_start((1, 1, 3, 1))
    x_wait(1, 1, 1, 0)
    x_start((1, 1, 2, 0), (1, 1, 1, 1))
    x_wait(1, 0, 2, 0)
    x_start((1, 0, 2, 1))
    x_wait(1, 1, 2, 0)
    x_start((1, 1, 2, 1))
    with jax.named_scope('fwd1'):
        w_forward(1)
    w_start(0, 2)
    for line in range(2):
        for mb in range(n_mb):
            for r in range(n_x):
                x_wait(line, mb, r, 1)
    for line in range(2):
        for r in range(n_x):
            for cc in range(2):
                if (line, r, cc) != (0, 0, 0):
                    p_copy(line, (n_x - r) % n_x, cc).wait_recv()
    for mb in range(n_mb):
        pltpu.make_async_copy(rows_v.at[mb], x_slot(0, mb, 0, 0), xsem.at[mb]).wait()

    n_unit = n_mb * 2 * n_blk
    place_i = lax.broadcasted_iota(jnp.int32, (cap, tok), 0).astype(jnp.float32)

    def x_load(u):
        slot = u % 2
        return pltpu.make_async_copy(xg_ref.at[u // (2 * n_blk), u % (2 * n_blk)], rows_v.at[slot], xsem.at[slot])

    def row_store(u):
        slot = u % 2
        mb, i = u // (2 * n_blk), u % (2 * n_blk)
        return pltpu.make_async_copy(send_v.at[slot], rb_ref.at[pl.ds(0, half), mb, i // n_blk, i % n_blk], ssem.at[slot])

    x_load(0).start()

    def dispatch(u, carry):
        slot = u % 2
        mb, i = u // (2 * n_blk), u % (2 * n_blk)
        x_load(u).wait()

        @pl.when(u + 1 < n_unit)
        def _():
            x_load(u + 1).start()

        pick = jnp.concatenate(
            [jnp.where(pl_v[i, pl.ds(mb * half + k, 1), :] == place_i, 1.0, 0.0) for k in range(half)], axis=0)
        pick = pick.astype(jnp.bfloat16)

        @pl.when(u >= 2)
        def _():
            row_store(u - 2).wait()

        def tile(n, carry):
            cols = pl.ds(pl.multiple_of(n * n_tile, n_tile), n_tile)
            block = rows_v[slot, :, :, cols].reshape(tok, n_tile)
            got = jnp.dot(pick, block, preferred_element_type=jnp.float32).astype(jnp.bfloat16)
            send_v[slot, :, :, cols] = got.reshape(half, cap, n_tile)
            return carry

        lax.fori_loop(0, d_model // n_tile, tile, 0)
        row_store(u).start()
        return carry

    with jax.named_scope('dispatch'):
        lax.fori_loop(0, n_unit, dispatch, 0)
    row_store(n_unit - 2).wait()
    row_store(n_unit - 1).wait()

    n_chunk = 2 * n_mb
    rows_chunk = n_blk * cap

    def chunk_of(ck):
        return 1 - ck // n_mb, ck % n_mb

    def row_load(k, ck):
        line, mb = chunk_of(ck)
        return pltpu.make_async_copy(rb_ref.at[k, mb, line], rows_v.at[ck % 2], rsem.at[ck % 2])

    def w_load(j, k, a):
        owner = (twin_d, part_d, 3 - twin_d, d)[j]
        at = pl.ds(pl.multiple_of(owner * d_loc, d_loc), d_loc)
        src = w_in[a].at[half * h + k] if j == 3 else w_land[a].at[j, k]
        dst = wd_v.at[:, at] if a == 2 else (wg_v, wu_v)[a].at[at, :]
        return pltpu.make_async_copy(src, dst, wl.at[j, a])

    def far_send(k, ck, rc):
        line, mb = chunk_of(ck)
        r, cc = rc // 2, rc % 2
        back = ((n_x - r) % n_x) * 2 + cc
        return remote(o_v.at[ck, rc], bk_ref.at[k, mb, line, back], bs.at[ck], br.at[k, ck], dev(line, r, cc))

    def near_send(k, ck):
        line, mb = chunk_of(ck)
        return remote(o_v.at[ck, 0], bk_ref.at[k, mb, line, 0], b0.at[ck], br0.at[k, mb], partner)

    def near_copy(k, ck):
        line, mb = chunk_of(ck)
        return pltpu.make_async_copy(o_v.at[ck, 0], bk_ref.at[k, mb, line, 0], b0.at[ck])

    def sent_wait(ck):
        many = o_v.at[ck, pl.ds(1, n_blk - 1)]
        pltpu.make_async_copy(many, many, bs.at[ck]).wait()
        one = o_v.at[ck, 0]
        pltpu.make_async_copy(one, one, b0.at[ck]).wait()

    def compute(k):
        row_load(k, 0).start()
        for a in range(3):
            w_load(3, k, a).start()
        for a in range(3):
            w_load(1, k, a).start()
        with jax.named_scope('wait_own'):
            for a in range(3):
                w_copy(0, k, a).wait_recv()
                w_load(0, k, a).start()
        with jax.named_scope('wait_up'):
            for a in range(2):
                w_copy(2, k, a).wait_recv()
                w_load(2, k, a).start()
            for j in range(4):
                for a in range(2):
                    w_load(j, k, a).wait()

        def up_chunk(ck, carry):
            slot = ck % 2
            row_load(k, ck).wait()

            @pl.when(ck + 1 < n_chunk)
            def _():
                row_load(k, ck + 1).start()

            def up_tile(f, carry):
                cols = pl.ds(pl.multiple_of(f * LANES, LANES), LANES)
                both = jnp.concatenate([wg_v[:, cols], wu_v[:, cols]], axis=1)
                pre = jnp.dot(rows_v[slot].reshape(rows_chunk, d_model), both, preferred_element_type=jnp.float32)
                h_v[ck, :, cols] = (jax.nn.silu(pre[:, :LANES]) * pre[:, LANES:]).astype(jnp.bfloat16)
                return carry

            lax.fori_loop(0, ff // LANES, up_tile, 0)
            return carry

        with jax.named_scope('up'):
            lax.fori_loop(0, n_chunk, up_chunk, 0)
        with jax.named_scope('wait_down'):
            w_copy(2, k, 2).wait_recv()
            w_load(2, k, 2).start()
            for j in range(4):
                w_load(j, k, 2).wait()

        def down_chunk(ck, carry):
            @pl.when(k > 0)
            def _():
                with jax.named_scope('wait_sent'):
                    sent_wait(ck)

            def down_tile(n, carry):
                cols = pl.ds(pl.multiple_of(n * n_tile, n_tile), n_tile)
                out = jnp.dot(h_v[ck], wd_v[:, cols], preferred_element_type=jnp.float32).astype(jnp.bfloat16)
                o_v[ck, :, :, cols] = out.reshape(n_blk, cap, n_tile)
                return carry

            lax.fori_loop(0, d_model // n_tile, down_tile, 0)

            @pl.when(ck < n_mb)
            def _():
                near_send(k, ck).start()

            @pl.when(ck >= n_mb)
            def _():
                near_copy(k, ck).start()

            for rc in range(1, n_blk):
                far_send(k, ck, rc).start()
            return carry

        with jax.named_scope('down'):
            lax.fori_loop(0, n_chunk, down_chunk, 0)

    n_grp = n_blk // 4
    k_rows = 4 * cap

    def mix_of(u):
        v = u // n_grp
        return v % 2, v // 2

    def o_load(k, u):
        line, mb = mix_of(u)
        return pltpu.make_async_copy(bk_ref.at[k, mb, line, pl.ds((u % n_grp) * 4, 4)], ob_v.at[u % 2], osem.at[u % 2])

    def o_ready(k, u):
        line, mb = mix_of(u)
        ck = (1 - line) * n_mb + mb

        @pl.when(u % n_grp == 0)
        def _():
            with jax.named_scope('wait_back'):
                many = bk_ref.at[k, mb, line, pl.ds(1, n_blk - 1)]
                pltpu.make_async_copy(many, many, br.at[k, ck]).wait()

        @pl.when(jnp.logical_and(u % n_grp == 0, line == 1))
        def _():
            with jax.named_scope('wait_near'):
                near_send(k, ck).wait_recv()

        o_load(k, u).start()

    def combine(k):
        o_ready(k, 0)

        def unit(u, carry):
            line, mb = mix_of(u)
            slot = u % 2
            parts = []
            for i in range(4):
                q = quad(line, (u % n_grp) * 4 + i)
                hit = p_v[q, pl.ds(mb * half + k, 1), :] == place_i
                parts.append(jnp.where(hit, g_v[q, pl.ds(mb * half + k, 1), :], 0.0))
            mix = jnp.concatenate(parts, axis=0).T
            first = mix.astype(jnp.bfloat16)
            rest = mix - first.astype(jnp.float32)
            second = rest.astype(jnp.bfloat16)
            third = (rest - second.astype(jnp.float32)).astype(jnp.bfloat16)
            lt_v[:, 0:k_rows] = first
            lt_v[:, k_rows:2 * k_rows] = second
            lt_v[:, 2 * k_rows:3 * k_rows] = third
            o_load(k, u).wait()

            @pl.when(u + 1 < n_chunk * n_grp)
            def _():
                o_ready(k, u + 1)

            def tile(n, carry):
                cols = pl.ds(pl.multiple_of(n * n_tile, n_tile), n_tile)
                rows = ob_v[slot, :, :, cols].reshape(k_rows, n_tile)
                acc_v[mb, :, cols] += jnp.dot(lt_v[...], jnp.concatenate([rows, rows, rows], axis=0),
                                              preferred_element_type=jnp.float32)
                return carry

            lax.fori_loop(0, d_model // n_tile, tile, 0)
            return carry

        lax.fori_loop(0, n_chunk * n_grp, unit, 0)

    def step(k, carry):
        @pl.when(k < half)
        def _():
            compute(k)

        @pl.when(k + 2 < half)
        def _():
            with jax.named_scope('fwd'):
                w_forward(k + 2)

        @pl.when(k + 3 < half)
        def _():
            w_start(0, k + 3)

        @pl.when(k == half)
        def _():
            with jax.named_scope('sent_last'):
                for ck in range(n_chunk):
                    sent_wait(ck)

        @pl.when(k > 0)
        def _():
            with jax.named_scope('combine'):
                combine(k - 1)

        return carry

    lax.fori_loop(0, half + 1, step, 0)

    for mb in range(n_mb):
        rows_v[mb] = acc_v[mb].astype(jnp.bfloat16).reshape(n_blk, cap, d_model)
        pltpu.make_async_copy(rows_v.at[mb], y_ref.at[mb], ysem.at[mb]).start()

    with jax.named_scope('drain'):
        for flow in range(3):
            for k in range(half):
                for a in range(3):
                    w_copy(flow, k, a).wait_send()
    for line in range(2):
        for mb in range(n_mb):
            for r in range(n_x):
                for cc in range(2):
                    if (line, r, cc) != (0, 0, 0):
                        x_copy(line, mb, r, cc).wait_send()
    for line in range(2):
        for r in range(n_x):
            for cc in range(2):
                if (line, r, cc) != (0, 0, 0):
                    p_copy(line, r, cc).wait_send()
    for mb in range(n_mb):
        pltpu.make_async_copy(rows_v.at[mb], y_ref.at[mb], ysem.at[mb]).wait()


def solution(mesh):
    expert_devs = mesh.shape['expert']
    n_x = expert_devs // 2
    row_spec = P(None, ('rep', 'expert', 'data'), None)
    up_spec = P('expert', 'data', None)
    down_spec = P('expert', None, 'data')

    def per_device(x_loc, idx_loc, gate_loc, wg_loc, wu_loc, wd_loc):
        n_mb, tok, d_model = x_loc.shape
        n_top = idx_loc.shape[2]
        n_loc, d_loc, ff = wg_loc.shape
        n_exp = n_loc * expert_devs
        half = n_loc // 2
        cap = 8 * ((5 * n_top * tok + 32 * n_exp - 1) // (32 * n_exp))
        assert tok == expert_devs * cap
        bf16, f32 = jnp.bfloat16, jnp.float32
        n_quad = 2 * expert_devs
        rows = (expert_devs, cap, d_model)
        hbm = pl.BlockSpec(memory_space=pl.ANY)
        vmem = pl.BlockSpec(memory_space=pltpu.VMEM)
        dma = pltpu.SemaphoreType.DMA
        out = pl.pallas_call(
            functools.partial(moe_kernel, n_x, cap),
            out_shape=[
                jax.ShapeDtypeStruct((n_mb,) + rows, bf16),
                jax.ShapeDtypeStruct((n_mb, n_quad) + rows, bf16),
                jax.ShapeDtypeStruct((half, n_mb, 2) + rows, bf16),
                jax.ShapeDtypeStruct((half, n_mb, 2) + rows, bf16),
                jax.ShapeDtypeStruct((3, half, d_loc, ff), bf16),
                jax.ShapeDtypeStruct((3, half, d_loc, ff), bf16),
                jax.ShapeDtypeStruct((3, half, ff, d_loc), bf16),
            ],
            in_specs=[hbm, vmem, vmem, hbm, hbm, hbm],
            out_specs=[hbm] * 7,
            scratch_shapes=[
                pltpu.VMEM((4 * d_loc, ff), bf16),
                pltpu.VMEM((4 * d_loc, ff), bf16),
                pltpu.VMEM((ff, 4 * d_loc), bf16),
                pltpu.VMEM((2,) + rows, bf16),
                pltpu.VMEM((2 * n_mb,) + rows, bf16),
                pltpu.VMEM((2 * n_mb, tok, ff), bf16),
                pltpu.VMEM((n_mb, tok, d_model), f32),
                pltpu.VMEM((2, half, cap, d_model), bf16),
                pltpu.VMEM((2, 4, cap, d_model), bf16),
                pltpu.VMEM((tok, 12 * cap), bf16),
                pltpu.VMEM((n_quad, n_mb * half, tok), f32),
                pltpu.VMEM((n_quad, n_mb * half, tok), f32),
                pltpu.VMEM((n_quad, n_mb * half, tok), f32),
                dma((3, half, 3)), dma((3, half, 3)), dma((4, 3)),
                dma((n_mb, n_quad)), dma((n_mb, n_quad)),
                dma((n_quad,)), dma((n_quad,)),
                dma((2,)), dma((2,)), dma((2,)),
                dma((2 * n_mb,)), dma((2 * n_mb,)),
                dma((half, 2 * n_mb)), dma((half, n_mb)),
                dma((2,)), dma((2,)),
            ],
            compiler_params=pltpu.CompilerParams(collective_id=0, has_side_effects=True, vmem_limit_bytes=62 * 1024 * 1024),
        )(x_loc.reshape((n_mb,) + rows), idx_loc.transpose(2, 0, 1), gate_loc.transpose(2, 0, 1), wg_loc, wu_loc, wd_loc)
        return out[0].reshape(n_mb, tok, d_model)

    return jax.shard_map(per_device, mesh=mesh, in_specs=(row_spec, row_spec, row_spec, up_spec, up_spec, down_spec),
                         out_specs=row_spec, check_vma=False)
```

```python
import functools

import jax
import jax.numpy as jnp
from jax import lax
from jax.experimental import pallas as pl
from jax.experimental.pallas import tpu as pltpu
from jax.sharding import PartitionSpec as P

MESH = pl.DeviceIdType.MESH
LANES = 128


def moe_kernel(n_x, cap, x_ref, ids_ref, gate_ref, wg_ref, wu_ref, wd_ref,
               y_ref, xg_ref, rb_ref, bk_ref, lg_ref, lu_ref, ld_ref,
               wg_v, wu_v, wd_v, rows_v, o_v, h_v, acc_v, send_v, ob_v, lt_v, p_v, g_v, pl_v,
               ws, wr, wl, xs, xr, ps, pr, xsem, ssem, rsem, bs, b0, br, br0, osem, ysem):
    n_mb, n_blk, _, d_model = x_ref.shape
    tok = n_blk * cap
    n_loc, d_loc, ff = wg_ref.shape
    half = n_loc // 2
    n_quad = n_blk * 2
    n_exp = n_blk * n_loc
    n_top = ids_ref.shape[0]
    n_tile = min(256, d_loc)
    n_part = d_loc // n_tile

    e = lax.axis_index('expert')
    d = lax.axis_index('data')
    x = e // 2
    c = e % 2
    h = d // 2
    twin_d = d + 1 - 2 * (d % 2)
    part_d = 3 - d

    def dev(line, r, cc):
        return {'expert': 2 * ((x + r) % n_x) + (c + cc) % 2, 'data': d + line * (part_d - d)}

    def quad(line, rc):
        r, cc = rc // 2, rc % 2
        return 2 * (2 * ((x + r) % n_x) + (c + cc) % 2) + (h + line * (1 - 2 * h))

    twin = {'expert': e, 'data': twin_d}
    partner = {'expert': e, 'data': part_d}
    self_q = quad(0, 0)

    peers = [dev(line, r, cc) for line in range(2) for r in range(n_x) for cc in range(2) if (line, r, cc) != (0, 0, 0)]
    barrier = pltpu.get_barrier_semaphore()
    for peer in peers + [twin]:
        pl.semaphore_signal(barrier, inc=1, device_id=peer, device_id_type=MESH)
    pl.semaphore_wait(barrier, len(peers) + 1)

    def remote(src, dst, send_sem, recv_sem, device):
        return pltpu.make_async_remote_copy(src_ref=src, dst_ref=dst, send_sem=send_sem, recv_sem=recv_sem,
                                            device_id=device, device_id_type=MESH)

    w_in = (wg_ref, wu_ref, wd_ref)
    w_land = (lg_ref, lu_ref, ld_ref)

    def w_copy(flow, k, a):
        if flow == 0:
            src, device = w_in[a].at[half * h + k], twin
        elif flow == 1:
            src, device = w_in[a].at[half * (1 - h) + k], partner
        else:
            src, device = w_land[a].at[1, k], twin
        return remote(src, w_land[a].at[flow, k], ws.at[flow, k, a], wr.at[flow, k, a], device)

    def w_start(flow, k):
        for a in range(3):
            w_copy(flow, k, a).start()

    def w_forward(k):
        for a in range(3):
            w_copy(1, k, a).wait_recv()
            w_copy(2, k, a).start()

    def x_slot(line, mb, r, cc):
        return xg_ref.at[mb, line * n_blk + r * 2 + cc]

    def x_have(line, mb, r):
        return x_ref.at[mb] if (line, r) == (0, 0) else x_slot(line, mb, r, 0)

    def x_copy(line, mb, r, cc):
        if cc == 1:
            src, device = x_have(line, mb, r), dev(0, 0, 1)
        elif r == 0:
            src, device = x_ref.at[mb], partner
        elif r == n_x - 1:
            src, device = x_have(line, mb, 0), dev(0, 1, 0)
        elif r == 1:
            src, device = x_have(line, mb, 0), dev(0, n_x - 1, 0)
        elif mb == 0:
            src, device = x_have(line, mb, n_x - 1), dev(0, 1, 0)
        else:
            src, device = x_have(line, mb, 1), dev(0, n_x - 1, 0)
        i = line * n_blk + r * 2 + cc
        return remote(src, x_slot(line, mb, r, cc), xs.at[mb, i], xr.at[mb, i], device)

    def x_start(*keys):
        for key in keys:
            x_copy(*key).start()

    def x_wait(*key):
        x_copy(*key).wait_recv()

    def p_copy(line, r, cc):
        rr = (n_x - r) % n_x
        i = line * n_blk + rr * 2 + cc
        return remote(p_v.at[quad(line, r * 2 + cc)], pl_v.at[i], ps.at[i], pr.at[i], dev(line, r, cc))

    w_start(0, 0)
    for mb in range(n_mb):
        x_start((1, mb, 0, 0), (0, mb, 3, 0), (0, mb, 1, 0), (0, mb, 0, 1))

    row_i = lax.broadcasted_iota(jnp.int32, (tok, tok), 0)
    col_i = lax.broadcasted_iota(jnp.int32, (tok, tok), 1)
    earlier = jnp.where(row_i < col_i, 1.0, 0.0).astype(jnp.bfloat16)
    exp_i = lax.broadcasted_iota(jnp.int32, (n_exp, tok), 0)
    for mb in range(n_mb):
        picked = jnp.zeros((n_exp, tok), jnp.float32)
        weight = jnp.zeros((n_exp, tok), jnp.float32)
        for j in range(n_top):
            match = exp_i == ids_ref[j, mb:mb + 1, :]
            picked = picked + jnp.where(match, 1.0, 0.0)
            weight = weight + jnp.where(match, gate_ref[j, mb:mb + 1, :], 0.0)
        place = jnp.dot(picked.astype(jnp.bfloat16), earlier, preferred_element_type=jnp.float32)
        slot_of = jnp.where(picked > 0.5, jnp.where(place < cap - 0.5, place, -1.0), -1.0)
        p_v[:, mb * half:(mb + 1) * half, :] = slot_of.reshape(n_quad, half, tok)
        g_v[:, mb * half:(mb + 1) * half, :] = weight.reshape(n_quad, half, tok)
    for line in range(2):
        for r in range(n_x):
            for cc in range(2):
                if (line, r, cc) != (0, 0, 0):
                    p_copy(line, r, cc).start()
    for k in range(1, half - 1):
        w_start(0, k)
    for k in range(half):
        w_start(1, k)
    pl_v[0] = p_v[self_q]

    for mb in range(n_mb):
        pltpu.make_async_copy(x_ref.at[mb], rows_v.at[mb], xsem.at[mb]).start()
    for mb in range(n_mb):
        pltpu.make_async_copy(x_ref.at[mb], rows_v.at[mb], xsem.at[mb]).wait()
        pltpu.make_async_copy(rows_v.at[mb], x_slot(0, mb, 0, 0), xsem.at[mb]).start()
        acc_v[mb] = rows_v[mb].reshape(tok, d_model).astype(jnp.float32)

    x_wait(0, 0, 3, 0)
    x_start((0, 0, 2, 0), (0, 0, 3, 1))
    x_wait(0, 0, 1, 0)
    x_start((0, 0, 1, 1))
    x_wait(1, 0, 0, 0)
    x_start((1, 0, 3, 0), (1, 0, 1, 0), (1, 0, 0, 1))
    x_wait(0, 1, 3, 0)
    x_start((0, 1, 3, 1))
    x_wait(0, 1, 1, 0)
    x_start((0, 1, 2, 0), (0, 1, 1, 1))
    x_wait(1, 1, 0, 0)
    x_start((1, 1, 3, 0), (1, 1, 1, 0), (1, 1, 0, 1))
    x_wait(0, 0, 2, 0)
    x_start((0, 0, 2, 1))
    x_wait(1, 0, 1, 0)
    x_start((1, 0, 1, 1))
    x_wait(1, 0, 3, 0)
    x_start((1, 0, 2, 0), (1, 0, 3, 1))
    x_wait(0, 1, 2, 0)
    x_start((0, 1, 2, 1))
    w_forward(0)
    x_wait(1, 1, 3, 0)
    x_start((1, 1, 3, 1))
    x_wait(1, 1, 1, 0)
    x_start((1, 1, 2, 0), (1, 1, 1, 1))
    x_wait(1, 0, 2, 0)
    x_start((1, 0, 2, 1))
    x_wait(1, 1, 2, 0)
    x_start((1, 1, 2, 1))
    w_forward(1)
    for line in range(2):
        for mb in range(n_mb):
            for r in range(n_x):
                x_wait(line, mb, r, 1)
    for line in range(2):
        for r in range(n_x):
            for cc in range(2):
                if (line, r, cc) != (0, 0, 0):
                    p_copy(line, (n_x - r) % n_x, cc).wait_recv()
    for mb in range(n_mb):
        pltpu.make_async_copy(rows_v.at[mb], x_slot(0, mb, 0, 0), xsem.at[mb]).wait()

    n_unit = n_mb * 2 * n_blk
    place_i = lax.broadcasted_iota(jnp.int32, (cap, tok), 0).astype(jnp.float32)

    def x_load(u):
        slot = u % 2
        return pltpu.make_async_copy(xg_ref.at[u // (2 * n_blk), u % (2 * n_blk)], rows_v.at[slot], xsem.at[slot])

    def row_store(u):
        slot = u % 2
        mb, i = u // (2 * n_blk), u % (2 * n_blk)
        return pltpu.make_async_copy(send_v.at[slot], rb_ref.at[pl.ds(0, half), mb, i // n_blk, i % n_blk], ssem.at[slot])

    x_load(0).start()

    def dispatch(u, carry):
        slot = u % 2
        mb, i = u // (2 * n_blk), u % (2 * n_blk)
        x_load(u).wait()

        @pl.when(u + 1 < n_unit)
        def _():
            x_load(u + 1).start()

        pick = jnp.concatenate(
            [jnp.where(pl_v[i, pl.ds(mb * half + k, 1), :] == place_i, 1.0, 0.0) for k in range(half)], axis=0)
        pick = pick.astype(jnp.bfloat16)

        @pl.when(u >= 2)
        def _():
            row_store(u - 2).wait()

        def tile(n, carry):
            cols = pl.ds(pl.multiple_of(n * n_tile, n_tile), n_tile)
            block = rows_v[slot, :, :, cols].reshape(tok, n_tile)
            got = jnp.dot(pick, block, preferred_element_type=jnp.float32).astype(jnp.bfloat16)
            send_v[slot, :, :, cols] = got.reshape(half, cap, n_tile)
            return carry

        lax.fori_loop(0, d_model // n_tile, tile, 0)
        row_store(u).start()
        return carry

    lax.fori_loop(0, n_unit, dispatch, 0)
    row_store(n_unit - 2).wait()
    row_store(n_unit - 1).wait()

    n_chunk = 2 * n_mb
    rows_chunk = n_blk * cap

    def chunk_of(ck):
        return 1 - ck // n_mb, ck % n_mb

    def row_load(k, ck):
        line, mb = chunk_of(ck)
        return pltpu.make_async_copy(rb_ref.at[k, mb, line], rows_v.at[ck % 2], rsem.at[ck % 2])

    def w_load(j, k, a):
        owner = (twin_d, part_d, 3 - twin_d, d)[j]
        at = pl.ds(pl.multiple_of(owner * d_loc, d_loc), d_loc)
        src = w_in[a].at[half * h + k] if j == 3 else w_land[a].at[j, k]
        dst = wd_v.at[(j + 1) % 4] if a == 2 else (wg_v, wu_v)[a].at[at, :]
        return pltpu.make_async_copy(src, dst, wl.at[j, a])

    first, last = pl.ds(0, 3), pl.ds(3, 1)

    def send(k, ck, cols):
        line, mb = chunk_of(ck)

        @pl.when(line == 1)
        def _():
            remote(o_v.at[ck, 0, cols], bk_ref.at[k, mb, 1, 0, cols], b0.at[ck], br0.at[k, mb], partner).start()

        @pl.when(line == 0)
        def _():
            pltpu.make_async_copy(o_v.at[ck, 0, cols], bk_ref.at[k, mb, 0, 0, cols], b0.at[ck]).start()

        for rc in range(1, n_blk):
            r, cc = rc // 2, rc % 2
            back = ((n_x - r) % n_x) * 2 + cc
            remote(o_v.at[ck, rc, cols], bk_ref.at[k, mb, line, back, cols], bs.at[ck], br.at[k, ck],
                   dev(line, r, cc)).start()

    def sent_wait(ck):
        many = o_v.at[ck, pl.ds(1, n_blk - 1)]
        pltpu.make_async_copy(many, many, bs.at[ck]).wait()
        one = o_v.at[ck, 0]
        pltpu.make_async_copy(one, one, b0.at[ck]).wait()

    def down(ck, begin, end):
        def tile(n, carry):
            part = n // n_part
            cols = pl.ds(pl.multiple_of((n % n_part) * n_tile, n_tile), n_tile)
            out = jnp.dot(h_v[ck], wd_v[part, :, cols], preferred_element_type=jnp.float32).astype(jnp.bfloat16)
            o_v[ck, :, part, :, cols] = out.reshape(n_blk, cap, n_tile)
            return carry

        lax.fori_loop(begin * n_part, end * n_part, tile, 0)

    def compute(k):
        row_load(k, 0).start()
        for a in range(3):
            w_load(3, k, a).start()
        for a in range(3):
            w_load(1, k, a).start()
        for a in range(3):
            w_copy(0, k, a).wait_recv()
            w_load(0, k, a).start()
        for a in range(2):
            w_copy(2, k, a).wait_recv()
            w_load(2, k, a).start()
        for j in range(4):
            for a in range(2):
                w_load(j, k, a).wait()

        def up_chunk(ck, carry):
            slot = ck % 2
            row_load(k, ck).wait()

            @pl.when(ck + 1 < n_chunk)
            def _():
                row_load(k, ck + 1).start()

            def up_tile(f, carry):
                cols = pl.ds(pl.multiple_of(f * LANES, LANES), LANES)
                both = jnp.concatenate([wg_v[:, cols], wu_v[:, cols]], axis=1)
                pre = jnp.dot(rows_v[slot].reshape(rows_chunk, d_model), both, preferred_element_type=jnp.float32)
                h_v[ck, :, cols] = (jax.nn.silu(pre[:, :LANES]) * pre[:, LANES:]).astype(jnp.bfloat16)
                return carry

            lax.fori_loop(0, ff // LANES, up_tile, 0)

            @pl.when(k > 0)
            def _():
                sent_wait(ck)

            down(ck, 0, 3)
            send(k, ck, first)
            return carry

        for j in (3, 0, 1):
            w_load(j, k, 2).wait()
        lax.fori_loop(0, n_chunk, up_chunk, 0)
        w_copy(2, k, 2).wait_recv()
        w_load(2, k, 2).start()
        w_load(2, k, 2).wait()

        def down_chunk(ck, carry):
            down(ck, 3, 4)
            send(k, ck, last)
            return carry

        lax.fori_loop(0, n_chunk, down_chunk, 0)

    n_grp = n_blk // 4
    k_rows = 4 * cap

    def mix_of(u):
        v = u // n_grp
        return v % 2, v // 2

    def o_load(k, u):
        line, mb = mix_of(u)
        return pltpu.make_async_copy(bk_ref.at[k, mb, line, pl.ds((u % n_grp) * 4, 4)], ob_v.at[u % 2], osem.at[u % 2])

    def o_ready(k, u):
        line, mb = mix_of(u)
        ck = (1 - line) * n_mb + mb

        @pl.when(u % n_grp == 0)
        def _():
            many = bk_ref.at[k, mb, line, pl.ds(1, n_blk - 1)]
            pltpu.make_async_copy(many, many, br.at[k, ck]).wait()

        @pl.when(jnp.logical_and(u % n_grp == 0, line == 1))
        def _():
            one = bk_ref.at[k, mb, line, 0]
            pltpu.make_async_copy(one, one, br0.at[k, mb]).wait()

        o_load(k, u).start()

    def combine(k):
        o_ready(k, 0)

        def unit(u, carry):
            line, mb = mix_of(u)
            slot = u % 2
            parts = []
            for i in range(4):
                q = quad(line, (u % n_grp) * 4 + i)
                hit = p_v[q, pl.ds(mb * half + k, 1), :] == place_i
                parts.append(jnp.where(hit, g_v[q, pl.ds(mb * half + k, 1), :], 0.0))
            mix = jnp.concatenate(parts, axis=0).T
            first = mix.astype(jnp.bfloat16)
            rest = mix - first.astype(jnp.float32)
            second = rest.astype(jnp.bfloat16)
            third = (rest - second.astype(jnp.float32)).astype(jnp.bfloat16)
            lt_v[:, 0:k_rows] = first
            lt_v[:, k_rows:2 * k_rows] = second
            lt_v[:, 2 * k_rows:3 * k_rows] = third
            o_load(k, u).wait()

            @pl.when((u + 1) % n_grp != 0)
            def _():
                o_ready(k, u + 1)

            d_src = d + line * (3 - 2 * d)

            def tile(n, carry):
                part = n // n_part
                owner = d_src + (part % 2) * (1 - 2 * (d_src % 2))
                owner = owner + (part // 2) * (3 - 2 * owner)
                cols = pl.ds(pl.multiple_of((n % n_part) * n_tile, n_tile), n_tile)
                rows = ob_v[slot, :, part, :, cols].reshape(k_rows, n_tile)
                at = pl.ds(pl.multiple_of(owner * d_loc + (n % n_part) * n_tile, n_tile), n_tile)
                acc_v[mb, :, at] += jnp.dot(lt_v[...], jnp.concatenate([rows, rows, rows], axis=0),
                                              preferred_element_type=jnp.float32)
                return carry

            lax.fori_loop(0, d_model // n_tile, tile, 0)

            @pl.when(jnp.logical_and((u + 1) % n_grp == 0, u + 1 < n_chunk * n_grp))
            def _():
                o_ready(k, u + 1)

            @pl.when(jnp.logical_and(k == half - 1, (u + 1) % (2 * n_grp) == 0))
            def _():
                rows_v[mb] = acc_v[mb].astype(jnp.bfloat16).reshape(n_blk, cap, d_model)
                pltpu.make_async_copy(rows_v.at[mb], y_ref.at[mb], ysem.at[mb]).start()

            return carry

        lax.fori_loop(0, n_chunk * n_grp, unit, 0)

    def step(k, carry):
        @pl.when(k < half)
        def _():
            compute(k)

        @pl.when(k + 2 < half)
        def _():
            w_forward(k + 2)

        @pl.when(k == 0)
        def _():
            w_start(0, half - 1)

        @pl.when(k == half)
        def _():
            for ck in range(n_chunk):
                sent_wait(ck)

        @pl.when(k > 0)
        def _():
            combine(k - 1)

        return carry

    lax.fori_loop(0, half + 1, step, 0)

    for flow in range(3):
        for k in range(half):
            for a in range(3):
                w_copy(flow, k, a).wait_send()
    for line in range(2):
        for mb in range(n_mb):
            for r in range(n_x):
                for cc in range(2):
                    if (line, r, cc) != (0, 0, 0):
                        x_copy(line, mb, r, cc).wait_send()
    for line in range(2):
        for r in range(n_x):
            for cc in range(2):
                if (line, r, cc) != (0, 0, 0):
                    p_copy(line, r, cc).wait_send()
    for mb in range(n_mb):
        pltpu.make_async_copy(rows_v.at[mb], y_ref.at[mb], ysem.at[mb]).wait()


def solution(mesh):
    expert_devs = mesh.shape['expert']
    n_x = expert_devs // 2
    row_spec = P(None, ('rep', 'expert', 'data'), None)
    up_spec = P('expert', 'data', None)
    down_spec = P('expert', None, 'data')

    def per_device(x_loc, idx_loc, gate_loc, wg_loc, wu_loc, wd_loc):
        n_mb, tok, d_model = x_loc.shape
        n_top = idx_loc.shape[2]
        n_loc, d_loc, ff = wg_loc.shape
        n_exp = n_loc * expert_devs
        half = n_loc // 2
        cap = 8 * ((5 * n_top * tok + 32 * n_exp - 1) // (32 * n_exp))
        assert tok == expert_devs * cap
        bf16, f32 = jnp.bfloat16, jnp.float32
        n_quad = 2 * expert_devs
        rows = (expert_devs, cap, d_model)
        shards = (expert_devs, 4, cap, d_loc)
        hbm = pl.BlockSpec(memory_space=pl.ANY)
        vmem = pl.BlockSpec(memory_space=pltpu.VMEM)
        dma = pltpu.SemaphoreType.DMA
        out = pl.pallas_call(
            functools.partial(moe_kernel, n_x, cap),
            out_shape=[
                jax.ShapeDtypeStruct((n_mb,) + rows, bf16),
                jax.ShapeDtypeStruct((n_mb, n_quad) + rows, bf16),
                jax.ShapeDtypeStruct((half, n_mb, 2) + rows, bf16),
                jax.ShapeDtypeStruct((half, n_mb, 2) + shards, bf16),
                jax.ShapeDtypeStruct((3, half, d_loc, ff), bf16),
                jax.ShapeDtypeStruct((3, half, d_loc, ff), bf16),
                jax.ShapeDtypeStruct((3, half, ff, d_loc), bf16),
            ],
            in_specs=[hbm, vmem, vmem, hbm, hbm, hbm],
            out_specs=[hbm] * 7,
            scratch_shapes=[
                pltpu.VMEM((4 * d_loc, ff), bf16),
                pltpu.VMEM((4 * d_loc, ff), bf16),
                pltpu.VMEM((4, ff, d_loc), bf16),
                pltpu.VMEM((2,) + rows, bf16),
                pltpu.VMEM((2 * n_mb,) + shards, bf16),
                pltpu.VMEM((2 * n_mb, tok, ff), bf16),
                pltpu.VMEM((n_mb, tok, d_model), f32),
                pltpu.VMEM((2, half, cap, d_model), bf16),
                pltpu.VMEM((2, 4, 4, cap, d_loc), bf16),
                pltpu.VMEM((tok, 12 * cap), bf16),
                pltpu.VMEM((n_quad, n_mb * half, tok), f32),
                pltpu.VMEM((n_quad, n_mb * half, tok), f32),
                pltpu.VMEM((n_quad, n_mb * half, tok), f32),
                dma((3, half, 3)), dma((3, half, 3)), dma((4, 3)),
                dma((n_mb, n_quad)), dma((n_mb, n_quad)),
                dma((n_quad,)), dma((n_quad,)),
                dma((2,)), dma((2,)), dma((2,)),
                dma((2 * n_mb,)), dma((2 * n_mb,)),
                dma((half, 2 * n_mb)), dma((half, n_mb)),
                dma((2,)), dma((2,)),
            ],
            compiler_params=pltpu.CompilerParams(collective_id=0, has_side_effects=True, vmem_limit_bytes=62 * 1024 * 1024),
        )(x_loc.reshape((n_mb,) + rows), idx_loc.transpose(2, 0, 1), gate_loc.transpose(2, 0, 1), wg_loc, wu_loc, wd_loc)
        return out[0].reshape(n_mb, tok, d_model)

    return jax.shard_map(per_device, mesh=mesh, in_specs=(row_spec, row_spec, row_spec, up_spec, up_spec, down_spec),
                         out_specs=row_spec, check_vma=False)
```

```python
import functools

import jax
import jax.numpy as jnp
from jax import lax
from jax.experimental import pallas as pl
from jax.experimental.pallas import tpu as pltpu
from jax.sharding import PartitionSpec as P

MESH = pl.DeviceIdType.MESH
LANES = 128


def moe_kernel(n_x, cap, x_ref, ids_ref, gate_ref, wg_ref, wu_ref, wd_ref,
               y_ref, xg_ref, rb_ref, bk_ref, st_ref, lg_ref, lu_ref, ld_ref,
               wg_v, wu_v, wd_v, rows_v, o_v, h_v, acc_v, send_v, ob_v, lt_v, p_v, g_v, pl_v,
               ws, wr, wl, xs, xr, ps, pr, xsem, ssem, rsem, bs, b0, br, br0, fr, fs, osem, ysem):
    n_mb, n_blk, _, d_model = x_ref.shape
    tok = n_blk * cap
    n_loc, d_loc, ff = wg_ref.shape
    half = n_loc // 2
    n_quad = n_blk * 2
    n_exp = n_blk * n_loc
    n_top = ids_ref.shape[0]
    n_tile = min(256, d_loc)
    n_part = d_loc // n_tile

    e = lax.axis_index('expert')
    d = lax.axis_index('data')
    x = e // 2
    c = e % 2
    h = d // 2
    twin_d = d + 1 - 2 * (d % 2)
    part_d = 3 - d

    def dev(line, r, cc):
        return {'expert': 2 * ((x + r) % n_x) + (c + cc) % 2, 'data': d + line * (part_d - d)}

    def quad(line, rc):
        r, cc = rc // 2, rc % 2
        return 2 * (2 * ((x + r) % n_x) + (c + cc) % 2) + (h + line * (1 - 2 * h))

    twin = {'expert': e, 'data': twin_d}
    partner = {'expert': e, 'data': part_d}
    self_q = quad(0, 0)

    peers = [dev(line, r, cc) for line in range(2) for r in range(n_x) for cc in range(2) if (line, r, cc) != (0, 0, 0)]
    barrier = pltpu.get_barrier_semaphore()
    for peer in peers + [twin]:
        pl.semaphore_signal(barrier, inc=1, device_id=peer, device_id_type=MESH)
    pl.semaphore_wait(barrier, len(peers) + 1)

    def remote(src, dst, send_sem, recv_sem, device):
        return pltpu.make_async_remote_copy(src_ref=src, dst_ref=dst, send_sem=send_sem, recv_sem=recv_sem,
                                            device_id=device, device_id_type=MESH)

    w_in = (wg_ref, wu_ref, wd_ref)
    w_land = (lg_ref, lu_ref, ld_ref)

    def w_copy(flow, k, a):
        if flow == 0:
            src, device = w_in[a].at[half * h + k], twin
        elif flow == 1:
            src, device = w_in[a].at[half * (1 - h) + k], partner
        else:
            src, device = w_land[a].at[1, k], twin
        return remote(src, w_land[a].at[flow, k], ws.at[flow, k, a], wr.at[flow, k, a], device)

    def w_start(flow, k):
        for a in range(3):
            w_copy(flow, k, a).start()

    def w_forward(k):
        for a in range(3):
            w_copy(1, k, a).wait_recv()
            w_copy(2, k, a).start()

    def x_slot(line, mb, r, cc):
        return xg_ref.at[mb, line * n_blk + r * 2 + cc]

    def x_have(line, mb, r):
        return x_ref.at[mb] if (line, r) == (0, 0) else x_slot(line, mb, r, 0)

    def x_copy(line, mb, r, cc):
        if cc == 1:
            src, device = x_have(line, mb, r), dev(0, 0, 1)
        elif r == 0:
            src, device = x_ref.at[mb], partner
        elif r == n_x - 1:
            src, device = x_have(line, mb, 0), dev(0, 1, 0)
        elif r == 1:
            src, device = x_have(line, mb, 0), dev(0, n_x - 1, 0)
        elif mb == 0:
            src, device = x_have(line, mb, n_x - 1), dev(0, 1, 0)
        else:
            src, device = x_have(line, mb, 1), dev(0, n_x - 1, 0)
        i = line * n_blk + r * 2 + cc
        return remote(src, x_slot(line, mb, r, cc), xs.at[mb, i], xr.at[mb, i], device)

    def x_start(*keys):
        for key in keys:
            x_copy(*key).start()

    def x_wait(*key):
        x_copy(*key).wait_recv()

    def p_copy(line, r, cc):
        rr = (n_x - r) % n_x
        i = line * n_blk + rr * 2 + cc
        return remote(p_v.at[quad(line, r * 2 + cc)], pl_v.at[i], ps.at[i], pr.at[i], dev(line, r, cc))

    w_start(0, 0)
    for mb in range(n_mb):
        x_start((1, mb, 0, 0), (0, mb, 3, 0), (0, mb, 1, 0), (0, mb, 0, 1))

    row_i = lax.broadcasted_iota(jnp.int32, (tok, tok), 0)
    col_i = lax.broadcasted_iota(jnp.int32, (tok, tok), 1)
    earlier = jnp.where(row_i < col_i, 1.0, 0.0).astype(jnp.bfloat16)
    exp_i = lax.broadcasted_iota(jnp.int32, (n_exp, tok), 0)
    for mb in range(n_mb):
        picked = jnp.zeros((n_exp, tok), jnp.float32)
        weight = jnp.zeros((n_exp, tok), jnp.float32)
        for j in range(n_top):
            match = exp_i == ids_ref[j, mb:mb + 1, :]
            picked = picked + jnp.where(match, 1.0, 0.0)
            weight = weight + jnp.where(match, gate_ref[j, mb:mb + 1, :], 0.0)
        place = jnp.dot(picked.astype(jnp.bfloat16), earlier, preferred_element_type=jnp.float32)
        slot_of = jnp.where(picked > 0.5, jnp.where(place < cap - 0.5, place, -1.0), -1.0)
        p_v[:, mb * half:(mb + 1) * half, :] = slot_of.reshape(n_quad, half, tok)
        g_v[:, mb * half:(mb + 1) * half, :] = weight.reshape(n_quad, half, tok)
    for line in range(2):
        for r in range(n_x):
            for cc in range(2):
                if (line, r, cc) != (0, 0, 0):
                    p_copy(line, r, cc).start()
    for k in range(1, half - 1):
        w_start(0, k)
    for k in range(half):
        w_start(1, k)
    pl_v[0] = p_v[self_q]

    for mb in range(n_mb):
        pltpu.make_async_copy(x_ref.at[mb], rows_v.at[mb], xsem.at[mb]).start()
    for mb in range(n_mb):
        pltpu.make_async_copy(x_ref.at[mb], rows_v.at[mb], xsem.at[mb]).wait()
        pltpu.make_async_copy(rows_v.at[mb], x_slot(0, mb, 0, 0), xsem.at[mb]).start()
        acc_v[mb] = rows_v[mb].reshape(tok, d_model).astype(jnp.float32)

    x_wait(0, 0, 3, 0)
    x_start((0, 0, 2, 0), (0, 0, 3, 1))
    x_wait(0, 0, 1, 0)
    x_start((0, 0, 1, 1))
    x_wait(1, 0, 0, 0)
    x_start((1, 0, 3, 0), (1, 0, 1, 0), (1, 0, 0, 1))
    x_wait(0, 1, 3, 0)
    x_start((0, 1, 3, 1))
    x_wait(0, 1, 1, 0)
    x_start((0, 1, 2, 0), (0, 1, 1, 1))
    x_wait(1, 1, 0, 0)
    x_start((1, 1, 3, 0), (1, 1, 1, 0), (1, 1, 0, 1))
    x_wait(0, 0, 2, 0)
    x_start((0, 0, 2, 1))
    x_wait(1, 0, 1, 0)
    x_start((1, 0, 1, 1))
    x_wait(1, 0, 3, 0)
    x_start((1, 0, 2, 0), (1, 0, 3, 1))
    x_wait(0, 1, 2, 0)
    x_start((0, 1, 2, 1))
    w_forward(0)
    x_wait(1, 1, 3, 0)
    x_start((1, 1, 3, 1))
    x_wait(1, 1, 1, 0)
    x_start((1, 1, 2, 0), (1, 1, 1, 1))
    x_wait(1, 0, 2, 0)
    x_start((1, 0, 2, 1))
    x_wait(1, 1, 2, 0)
    x_start((1, 1, 2, 1))
    w_forward(1)
    for line in range(2):
        for mb in range(n_mb):
            for r in range(n_x):
                x_wait(line, mb, r, 1)
    for line in range(2):
        for r in range(n_x):
            for cc in range(2):
                if (line, r, cc) != (0, 0, 0):
                    p_copy(line, (n_x - r) % n_x, cc).wait_recv()
    for mb in range(n_mb):
        pltpu.make_async_copy(rows_v.at[mb], x_slot(0, mb, 0, 0), xsem.at[mb]).wait()

    n_unit = n_mb * 2 * n_blk
    place_i = lax.broadcasted_iota(jnp.int32, (cap, tok), 0).astype(jnp.float32)

    def x_load(u):
        slot = u % 2
        return pltpu.make_async_copy(xg_ref.at[u // (2 * n_blk), u % (2 * n_blk)], rows_v.at[slot], xsem.at[slot])

    def row_store(u):
        slot = u % 2
        mb, i = u // (2 * n_blk), u % (2 * n_blk)
        return pltpu.make_async_copy(send_v.at[slot], rb_ref.at[pl.ds(0, half), mb, i // n_blk, i % n_blk], ssem.at[slot])

    x_load(0).start()

    def dispatch(u, carry):
        slot = u % 2
        mb, i = u // (2 * n_blk), u % (2 * n_blk)
        x_load(u).wait()

        @pl.when(u + 1 < n_unit)
        def _():
            x_load(u + 1).start()

        pick = jnp.concatenate(
            [jnp.where(pl_v[i, pl.ds(mb * half + k, 1), :] == place_i, 1.0, 0.0) for k in range(half)], axis=0)
        pick = pick.astype(jnp.bfloat16)

        @pl.when(u >= 2)
        def _():
            row_store(u - 2).wait()

        def tile(n, carry):
            cols = pl.ds(pl.multiple_of(n * n_tile, n_tile), n_tile)
            block = rows_v[slot, :, :, cols].reshape(tok, n_tile)
            got = jnp.dot(pick, block, preferred_element_type=jnp.float32).astype(jnp.bfloat16)
            send_v[slot, :, :, cols] = got.reshape(half, cap, n_tile)
            return carry

        lax.fori_loop(0, d_model // n_tile, tile, 0)
        row_store(u).start()
        return carry

    lax.fori_loop(0, n_unit, dispatch, 0)
    row_store(n_unit - 2).wait()
    row_store(n_unit - 1).wait()

    n_chunk = 2 * n_mb
    rows_chunk = n_blk * cap

    def chunk_of(ck):
        return 1 - ck // n_mb, ck % n_mb

    def row_load(k, ck):
        line, mb = chunk_of(ck)
        return pltpu.make_async_copy(rb_ref.at[k, mb, line], rows_v.at[ck % 2], rsem.at[ck % 2])

    def w_load(j, k, a):
        owner = (twin_d, part_d, 3 - twin_d, d)[j]
        at = pl.ds(pl.multiple_of(owner * d_loc, d_loc), d_loc)
        src = w_in[a].at[half * h + k] if j == 3 else w_land[a].at[j, k]
        dst = wd_v.at[(j + 1) % 4] if a == 2 else (wg_v, wu_v)[a].at[at, :]
        return pltpu.make_async_copy(src, dst, wl.at[j, a])

    first, last = pl.ds(0, 3), pl.ds(3, 1)

    def send(k, ck, cols):
        line, mb = chunk_of(ck)

        @pl.when(line == 1)
        def _():
            remote(o_v.at[ck, 0, cols], bk_ref.at[k, mb, 1, 0, cols], b0.at[ck], br0.at[k, mb], partner).start()

        @pl.when(line == 0)
        def _():
            pltpu.make_async_copy(o_v.at[ck, 0, cols], bk_ref.at[k, mb, 0, 0, cols], b0.at[ck]).start()

        @pl.when(line == 1)
        def _():
            relay(k, mb, cols).start()

        @pl.when(line == 0)
        def _():
            for rc in range(1, n_blk):
                remote(o_v.at[ck, rc, cols], bk_ref.at[k, mb, 0, back_of(rc), cols], bs.at[ck], br.at[k, ck],
                       dev(0, rc // 2, rc % 2)).start()

    def back_of(rc):
        return ((n_x - rc // 2) % n_x) * 2 + rc % 2

    def relay(k, mb, cols):
        phase = 0 if cols is first else 1
        return remote(o_v.at[mb, pl.ds(1, n_blk - 1), cols], st_ref.at[k, mb, pl.ds(0, n_blk - 1), cols], bs.at[mb],
                      fr.at[k, mb, phase], partner)

    def relay_on(k, mb, cols):
        relay(k, mb, cols).wait_recv()
        for rc in range(1, n_blk):
            remote(st_ref.at[k, mb, rc - 1, cols], bk_ref.at[k, mb, 1, back_of(rc), cols], fs.at[k, mb], br.at[k, mb],
                   dev(0, rc // 2, rc % 2)).start()

    def sent_wait(ck):
        many = o_v.at[ck, pl.ds(1, n_blk - 1)]
        pltpu.make_async_copy(many, many, bs.at[ck]).wait()
        one = o_v.at[ck, 0]
        pltpu.make_async_copy(one, one, b0.at[ck]).wait()

    def down(ck, begin, end):
        def tile(n, carry):
            part = n // n_part
            cols = pl.ds(pl.multiple_of((n % n_part) * n_tile, n_tile), n_tile)
            out = jnp.dot(h_v[ck], wd_v[part, :, cols], preferred_element_type=jnp.float32).astype(jnp.bfloat16)
            o_v[ck, :, part, :, cols] = out.reshape(n_blk, cap, n_tile)
            return carry

        lax.fori_loop(begin * n_part, end * n_part, tile, 0)

    def relay_rest(k):
        for mb in range(1, n_mb):
            relay_on(k, mb, first)
        for mb in range(n_mb):
            relay_on(k, mb, last)

    def compute(k):
        row_load(k, 0).start()
        for a in range(3):
            w_load(3, k, a).start()
        for a in range(3):
            w_load(1, k, a).start()
        for a in range(3):
            w_copy(0, k, a).wait_recv()
            w_load(0, k, a).start()

        @pl.when(k > 0)
        def _():
            relay_on(k - 1, 0, first)

        for a in range(2):
            w_copy(2, k, a).wait_recv()
            w_load(2, k, a).start()
        for j in range(4):
            for a in range(2):
                w_load(j, k, a).wait()

        def up_chunk(ck, carry):
            slot = ck % 2
            row_load(k, ck).wait()

            @pl.when(ck + 1 < n_chunk)
            def _():
                row_load(k, ck + 1).start()

            def up_tile(f, carry):
                cols = pl.ds(pl.multiple_of(f * LANES, LANES), LANES)
                both = jnp.concatenate([wg_v[:, cols], wu_v[:, cols]], axis=1)
                pre = jnp.dot(rows_v[slot].reshape(rows_chunk, d_model), both, preferred_element_type=jnp.float32)
                h_v[ck, :, cols] = (jax.nn.silu(pre[:, :LANES]) * pre[:, LANES:]).astype(jnp.bfloat16)
                return carry

            lax.fori_loop(0, ff // LANES, up_tile, 0)

            @pl.when(k > 0)
            def _():
                sent_wait(ck)

            down(ck, 0, 3)
            send(k, ck, first)
            return carry

        for j in (3, 0, 1):
            w_load(j, k, 2).wait()
        lax.fori_loop(0, n_chunk, up_chunk, 0)

        @pl.when(k > 0)
        def _():
            relay_rest(k - 1)

        w_copy(2, k, 2).wait_recv()
        w_load(2, k, 2).start()
        w_load(2, k, 2).wait()

        def down_chunk(ck, carry):
            down(ck, 3, 4)
            send(k, ck, last)
            return carry

        lax.fori_loop(0, n_chunk, down_chunk, 0)

    n_grp = n_blk // 4
    k_rows = 4 * cap

    def mix_of(u):
        v = u // n_grp
        return v // n_mb, v % n_mb

    def o_load(k, u):
        line, mb = mix_of(u)
        return pltpu.make_async_copy(bk_ref.at[k, mb, line, pl.ds((u % n_grp) * 4, 4)], ob_v.at[u % 2], osem.at[u % 2])

    def o_ready(k, u):
        line, mb = mix_of(u)
        ck = (1 - line) * n_mb + mb

        @pl.when(u % n_grp == 0)
        def _():
            many = bk_ref.at[k, mb, line, pl.ds(1, n_blk - 1)]
            pltpu.make_async_copy(many, many, br.at[k, ck]).wait()

        @pl.when(jnp.logical_and(u % n_grp == 0, line == 1))
        def _():
            one = bk_ref.at[k, mb, line, 0]
            pltpu.make_async_copy(one, one, br0.at[k, mb]).wait()

        o_load(k, u).start()

    def combine(k):
        @pl.when(k == half - 1)
        def _():
            relay_on(k, 0, first)

        o_ready(k, 0)

        def unit(u, carry):
            line, mb = mix_of(u)
            slot = u % 2
            parts = []
            for i in range(4):
                q = quad(line, (u % n_grp) * 4 + i)
                hit = p_v[q, pl.ds(mb * half + k, 1), :] == place_i
                parts.append(jnp.where(hit, g_v[q, pl.ds(mb * half + k, 1), :], 0.0))
            mix = jnp.concatenate(parts, axis=0).T
            first = mix.astype(jnp.bfloat16)
            rest = mix - first.astype(jnp.float32)
            second = rest.astype(jnp.bfloat16)
            third = (rest - second.astype(jnp.float32)).astype(jnp.bfloat16)
            lt_v[:, 0:k_rows] = first
            lt_v[:, k_rows:2 * k_rows] = second
            lt_v[:, 2 * k_rows:3 * k_rows] = third
            o_load(k, u).wait()

            @pl.when((u + 1) % n_grp != 0)
            def _():
                o_ready(k, u + 1)

            d_src = d + line * (3 - 2 * d)

            def tile(n, carry):
                part = n // n_part
                owner = d_src + (part % 2) * (1 - 2 * (d_src % 2))
                owner = owner + (part // 2) * (3 - 2 * owner)
                cols = pl.ds(pl.multiple_of((n % n_part) * n_tile, n_tile), n_tile)
                rows = ob_v[slot, :, part, :, cols].reshape(k_rows, n_tile)
                at = pl.ds(pl.multiple_of(owner * d_loc + (n % n_part) * n_tile, n_tile), n_tile)
                acc_v[mb, :, at] += jnp.dot(lt_v[...], jnp.concatenate([rows, rows, rows], axis=0),
                                              preferred_element_type=jnp.float32)
                return carry

            lax.fori_loop(0, d_model // n_tile, tile, 0)

            @pl.when(jnp.logical_and(k == half - 1, jnp.logical_and(line == 1, (u + 1) % n_grp == 0)))
            def _():
                rows_v[mb] = acc_v[mb].astype(jnp.bfloat16).reshape(n_blk, cap, d_model)
                pltpu.make_async_copy(rows_v.at[mb], y_ref.at[mb], ysem.at[mb]).start()

            @pl.when(jnp.logical_and(k == half - 1, u + 1 == n_mb * n_grp))
            def _():
                relay_rest(k)

            @pl.when(jnp.logical_and((u + 1) % n_grp == 0, u + 1 < n_chunk * n_grp))
            def _():
                o_ready(k, u + 1)

            return carry

        lax.fori_loop(0, n_chunk * n_grp, unit, 0)

    def step(k, carry):
        @pl.when(k < half)
        def _():
            compute(k)

        @pl.when(k + 2 < half)
        def _():
            w_forward(k + 2)

        @pl.when(k == 0)
        def _():
            w_start(0, half - 1)

        @pl.when(k == half)
        def _():
            for ck in range(n_chunk):
                sent_wait(ck)

        @pl.when(k > 0)
        def _():
            combine(k - 1)

        return carry

    lax.fori_loop(0, half + 1, step, 0)

    for k in range(half):
        for mb in range(n_mb):
            many = st_ref.at[k, mb]
            pltpu.make_async_copy(many, many, fs.at[k, mb]).wait()
    for flow in range(3):
        for k in range(half):
            for a in range(3):
                w_copy(flow, k, a).wait_send()
    for line in range(2):
        for mb in range(n_mb):
            for r in range(n_x):
                for cc in range(2):
                    if (line, r, cc) != (0, 0, 0):
                        x_copy(line, mb, r, cc).wait_send()
    for line in range(2):
        for r in range(n_x):
            for cc in range(2):
                if (line, r, cc) != (0, 0, 0):
                    p_copy(line, r, cc).wait_send()
    for mb in range(n_mb):
        pltpu.make_async_copy(rows_v.at[mb], y_ref.at[mb], ysem.at[mb]).wait()


def solution(mesh):
    expert_devs = mesh.shape['expert']
    n_x = expert_devs // 2
    row_spec = P(None, ('rep', 'expert', 'data'), None)
    up_spec = P('expert', 'data', None)
    down_spec = P('expert', None, 'data')

    def per_device(x_loc, idx_loc, gate_loc, wg_loc, wu_loc, wd_loc):
        n_mb, tok, d_model = x_loc.shape
        n_top = idx_loc.shape[2]
        n_loc, d_loc, ff = wg_loc.shape
        n_exp = n_loc * expert_devs
        half = n_loc // 2
        cap = 8 * ((5 * n_top * tok + 32 * n_exp - 1) // (32 * n_exp))
        assert tok == expert_devs * cap
        bf16, f32 = jnp.bfloat16, jnp.float32
        n_quad = 2 * expert_devs
        rows = (expert_devs, cap, d_model)
        shards = (expert_devs, 4, cap, d_loc)
        hbm = pl.BlockSpec(memory_space=pl.ANY)
        vmem = pl.BlockSpec(memory_space=pltpu.VMEM)
        dma = pltpu.SemaphoreType.DMA
        out = pl.pallas_call(
            functools.partial(moe_kernel, n_x, cap),
            out_shape=[
                jax.ShapeDtypeStruct((n_mb,) + rows, bf16),
                jax.ShapeDtypeStruct((n_mb, n_quad) + rows, bf16),
                jax.ShapeDtypeStruct((half, n_mb, 2) + rows, bf16),
                jax.ShapeDtypeStruct((half, n_mb, 2) + shards, bf16),
                jax.ShapeDtypeStruct((half, n_mb, expert_devs - 1) + shards[1:], bf16),
                jax.ShapeDtypeStruct((3, half, d_loc, ff), bf16),
                jax.ShapeDtypeStruct((3, half, d_loc, ff), bf16),
                jax.ShapeDtypeStruct((3, half, ff, d_loc), bf16),
            ],
            in_specs=[hbm, vmem, vmem, hbm, hbm, hbm],
            out_specs=[hbm] * 8,
            scratch_shapes=[
                pltpu.VMEM((4 * d_loc, ff), bf16),
                pltpu.VMEM((4 * d_loc, ff), bf16),
                pltpu.VMEM((4, ff, d_loc), bf16),
                pltpu.VMEM((2,) + rows, bf16),
                pltpu.VMEM((2 * n_mb,) + shards, bf16),
                pltpu.VMEM((2 * n_mb, tok, ff), bf16),
                pltpu.VMEM((n_mb, tok, d_model), f32),
                pltpu.VMEM((2, half, cap, d_model), bf16),
                pltpu.VMEM((2, 4, 4, cap, d_loc), bf16),
                pltpu.VMEM((tok, 12 * cap), bf16),
                pltpu.VMEM((n_quad, n_mb * half, tok), f32),
                pltpu.VMEM((n_quad, n_mb * half, tok), f32),
                pltpu.VMEM((n_quad, n_mb * half, tok), f32),
                dma((3, half, 3)), dma((3, half, 3)), dma((4, 3)),
                dma((n_mb, n_quad)), dma((n_mb, n_quad)),
                dma((n_quad,)), dma((n_quad,)),
                dma((2,)), dma((2,)), dma((2,)),
                dma((2 * n_mb,)), dma((2 * n_mb,)),
                dma((half, 2 * n_mb)), dma((half, n_mb)), dma((half, n_mb, 2)), dma((half, n_mb)),
                dma((2,)), dma((2,)),
            ],
            compiler_params=pltpu.CompilerParams(collective_id=0, has_side_effects=True, vmem_limit_bytes=62 * 1024 * 1024),
        )(x_loc.reshape((n_mb,) + rows), idx_loc.transpose(2, 0, 1), gate_loc.transpose(2, 0, 1), wg_loc, wu_loc, wd_loc)
        return out[0].reshape(n_mb, tok, d_model)

    return jax.shard_map(per_device, mesh=mesh, in_specs=(row_spec, row_spec, row_spec, up_spec, up_spec, down_spec),
                         out_specs=row_spec, check_vma=False)
```

```python
import functools

import jax
import jax.numpy as jnp
from jax import lax
from jax.experimental import pallas as pl
from jax.experimental.pallas import tpu as pltpu
from jax.sharding import PartitionSpec as P

MESH = pl.DeviceIdType.MESH
LANES = 128


def moe_kernel(n_x, cap, x_ref, ids_ref, gate_ref, wg_ref, wu_ref, wd_ref,
               y_ref, xg_ref, rb_ref, bk_ref, lg_ref, lu_ref, ld_ref,
               wg_v, wu_v, wd_v, rows_v, o_v, h_v, acc_v, send_v, ob_v, lt_v, p_v, g_v, pl_v,
               ws, wr, wl, xs, xr, ps, pr, xsem, ssem, rsem, bs, b0, br, br0, osem, ysem):
    n_mb, n_blk, _, d_model = x_ref.shape
    tok = n_blk * cap
    n_loc, d_loc, ff = wg_ref.shape
    half = n_loc // 2
    n_quad = n_blk * 2
    n_exp = n_blk * n_loc
    n_top = ids_ref.shape[0]
    n_tile = min(256, d_loc)
    n_part = d_loc // n_tile

    e = lax.axis_index('expert')
    d = lax.axis_index('data')
    x = e // 2
    c = e % 2
    h = d // 2
    twin_d = d + 1 - 2 * (d % 2)
    part_d = 3 - d

    def dev(line, r, cc):
        return {'expert': 2 * ((x + r) % n_x) + (c + cc) % 2, 'data': d + line * (part_d - d)}

    def quad(line, rc):
        r, cc = rc // 2, rc % 2
        return 2 * (2 * ((x + r) % n_x) + (c + cc) % 2) + (h + line * (1 - 2 * h))

    twin = {'expert': e, 'data': twin_d}
    partner = {'expert': e, 'data': part_d}
    self_q = quad(0, 0)

    peers = [dev(line, r, cc) for line in range(2) for r in range(n_x) for cc in range(2) if (line, r, cc) != (0, 0, 0)]
    barrier = pltpu.get_barrier_semaphore()
    for peer in peers + [twin]:
        pl.semaphore_signal(barrier, inc=1, device_id=peer, device_id_type=MESH)
    pl.semaphore_wait(barrier, len(peers) + 1)

    def remote(src, dst, send_sem, recv_sem, device):
        return pltpu.make_async_remote_copy(src_ref=src, dst_ref=dst, send_sem=send_sem, recv_sem=recv_sem,
                                            device_id=device, device_id_type=MESH)

    w_in = (wg_ref, wu_ref, wd_ref)
    w_land = (lg_ref, lu_ref, ld_ref)

    def w_copy(flow, k, a):
        if flow == 0:
            src, device = w_in[a].at[half * h + k], twin
        elif flow == 1:
            src, device = w_in[a].at[half * (1 - h) + k], partner
        else:
            src, device = w_land[a].at[1, k], twin
        return remote(src, w_land[a].at[flow, k], ws.at[flow, k, a], wr.at[flow, k, a], device)

    def w_start(flow, k):
        for a in range(3):
            w_copy(flow, k, a).start()

    def w_forward(k):
        for a in range(3):
            w_copy(1, k, a).wait_recv()
            w_copy(2, k, a).start()

    def x_slot(line, mb, r, cc):
        return xg_ref.at[mb, line * n_blk + r * 2 + cc]

    def x_have(line, mb, r):
        return x_ref.at[mb] if (line, r) == (0, 0) else x_slot(line, mb, r, 0)

    def x_copy(line, mb, r, cc):
        if cc == 1:
            src, device = x_have(line, mb, r), dev(0, 0, 1)
        elif r == 0:
            src, device = x_ref.at[mb], partner
        elif r == n_x - 1:
            src, device = x_have(line, mb, 0), dev(0, 1, 0)
        elif r == 1:
            src, device = x_have(line, mb, 0), dev(0, n_x - 1, 0)
        elif mb == 0:
            src, device = x_have(line, mb, n_x - 1), dev(0, 1, 0)
        else:
            src, device = x_have(line, mb, 1), dev(0, n_x - 1, 0)
        i = line * n_blk + r * 2 + cc
        return remote(src, x_slot(line, mb, r, cc), xs.at[mb, i], xr.at[mb, i], device)

    def x_start(*keys):
        for key in keys:
            x_copy(*key).start()

    def x_wait(*key):
        x_copy(*key).wait_recv()

    def p_copy(line, r, cc):
        rr = (n_x - r) % n_x
        i = line * n_blk + rr * 2 + cc
        return remote(p_v.at[quad(line, r * 2 + cc)], pl_v.at[i], ps.at[i], pr.at[i], dev(line, r, cc))

    w_start(0, 0)
    for mb in range(n_mb):
        x_start((1, mb, 0, 0), (0, mb, 3, 0), (0, mb, 1, 0), (0, mb, 0, 1))

    row_i = lax.broadcasted_iota(jnp.int32, (tok, tok), 0)
    col_i = lax.broadcasted_iota(jnp.int32, (tok, tok), 1)
    earlier = jnp.where(row_i < col_i, 1.0, 0.0).astype(jnp.bfloat16)
    exp_i = lax.broadcasted_iota(jnp.int32, (n_exp, tok), 0)
    for mb in range(n_mb):
        picked = jnp.zeros((n_exp, tok), jnp.float32)
        weight = jnp.zeros((n_exp, tok), jnp.float32)
        for j in range(n_top):
            match = exp_i == ids_ref[j, mb:mb + 1, :]
            picked = picked + jnp.where(match, 1.0, 0.0)
            weight = weight + jnp.where(match, gate_ref[j, mb:mb + 1, :], 0.0)
        place = jnp.dot(picked.astype(jnp.bfloat16), earlier, preferred_element_type=jnp.float32)
        slot_of = jnp.where(picked > 0.5, jnp.where(place < cap - 0.5, place, -1.0), -1.0)
        p_v[:, mb * half:(mb + 1) * half, :] = slot_of.reshape(n_quad, half, tok)
        g_v[:, mb * half:(mb + 1) * half, :] = weight.reshape(n_quad, half, tok)
    for line in range(2):
        for r in range(n_x):
            for cc in range(2):
                if (line, r, cc) != (0, 0, 0):
                    p_copy(line, r, cc).start()
    for k in range(1, half - 1):
        w_start(0, k)
    for k in range(half):
        w_start(1, k)
    pl_v[0] = p_v[self_q]

    for mb in range(n_mb):
        pltpu.make_async_copy(x_ref.at[mb], rows_v.at[mb], xsem.at[mb]).start()
    for mb in range(n_mb):
        pltpu.make_async_copy(x_ref.at[mb], rows_v.at[mb], xsem.at[mb]).wait()
        pltpu.make_async_copy(rows_v.at[mb], x_slot(0, mb, 0, 0), xsem.at[mb]).start()
        acc_v[mb] = rows_v[mb].reshape(tok, d_model).astype(jnp.float32)

    for mb in range(n_mb):
        for r in (3, 1):
            x_wait(0, mb, r, 0)
            if r == 3 - 2 * mb:
                x_start((0, mb, 2, 0))
            x_start((0, mb, r, 1))
        x_wait(1, mb, 0, 0)
        x_start((1, mb, 3, 0), (1, mb, 1, 0), (1, mb, 0, 1))
    x_wait(0, 0, 2, 0)
    x_start((0, 0, 2, 1))
    x_wait(1, 0, 1, 0)
    x_start((1, 0, 1, 1))
    x_wait(1, 0, 3, 0)
    x_start((1, 0, 2, 0), (1, 0, 3, 1))
    x_wait(0, 1, 2, 0)
    x_start((0, 1, 2, 1))
    w_forward(0)
    x_wait(1, 1, 3, 0)
    x_start((1, 1, 3, 1))
    x_wait(1, 1, 1, 0)
    x_start((1, 1, 2, 0), (1, 1, 1, 1))
    x_wait(1, 0, 2, 0)
    x_start((1, 0, 2, 1))
    x_wait(1, 1, 2, 0)
    x_start((1, 1, 2, 1))
    w_forward(1)
    for line in range(2):
        for mb in range(n_mb):
            for r in range(n_x):
                x_wait(line, mb, r, 1)
    for line in range(2):
        for r in range(n_x):
            for cc in range(2):
                if (line, r, cc) != (0, 0, 0):
                    p_copy(line, (n_x - r) % n_x, cc).wait_recv()
    for mb in range(n_mb):
        pltpu.make_async_copy(rows_v.at[mb], x_slot(0, mb, 0, 0), xsem.at[mb]).wait()

    n_unit = n_mb * 2 * n_blk
    place_i = lax.broadcasted_iota(jnp.int32, (cap, tok), 0).astype(jnp.float32)

    def x_load(u):
        slot = u % 2
        return pltpu.make_async_copy(xg_ref.at[u // (2 * n_blk), u % (2 * n_blk)], rows_v.at[slot], xsem.at[slot])

    def row_store(u):
        slot = u % 2
        mb, i = u // (2 * n_blk), u % (2 * n_blk)
        return pltpu.make_async_copy(send_v.at[slot], rb_ref.at[pl.ds(0, half), mb, i // n_blk, i % n_blk], ssem.at[slot])

    x_load(0).start()

    def dispatch(u, carry):
        slot = u % 2
        mb, i = u // (2 * n_blk), u % (2 * n_blk)
        x_load(u).wait()

        @pl.when(u + 1 < n_unit)
        def _():
            x_load(u + 1).start()

        pick = jnp.concatenate(
            [jnp.where(pl_v[i, pl.ds(mb * half + k, 1), :] == place_i, 1.0, 0.0) for k in range(half)], axis=0)
        pick = pick.astype(jnp.bfloat16)

        @pl.when(u >= 2)
        def _():
            row_store(u - 2).wait()

        def tile(n, carry):
            cols = pl.ds(pl.multiple_of(n * n_tile, n_tile), n_tile)
            block = rows_v[slot, :, :, cols].reshape(tok, n_tile)
            got = jnp.dot(pick, block, preferred_element_type=jnp.float32).astype(jnp.bfloat16)
            send_v[slot, :, :, cols] = got.reshape(half, cap, n_tile)
            return carry

        lax.fori_loop(0, d_model // n_tile, tile, 0)
        row_store(u).start()
        return carry

    lax.fori_loop(0, n_unit, dispatch, 0)
    row_store(n_unit - 2).wait()
    row_store(n_unit - 1).wait()

    n_chunk = 2 * n_mb
    rows_chunk = n_blk * cap

    def chunk_of(ck):
        return 1 - ck // n_mb, ck % n_mb

    def row_load(k, ck):
        line, mb = chunk_of(ck)
        return pltpu.make_async_copy(rb_ref.at[k, mb, line], rows_v.at[ck % 2], rsem.at[ck % 2])

    def w_load(j, k, a):
        owner = (twin_d, part_d, 3 - twin_d, d)[j]
        at = pl.ds(pl.multiple_of(owner * d_loc, d_loc), d_loc)
        src = w_in[a].at[half * h + k] if j == 3 else w_land[a].at[j, k]
        dst = wd_v.at[(j + 1) % 4] if a == 2 else (wg_v, wu_v)[a].at[at, :]
        return pltpu.make_async_copy(src, dst, wl.at[j, a])

    parts = pl.ds(0, 3), pl.ds(3, 1)

    def send(k, ck, part):
        line, mb = chunk_of(ck)
        cols = parts[part]

        @pl.when(line == 1)
        def _():
            remote(o_v.at[ck, 0, cols], bk_ref.at[k, mb, 1, 0, cols], b0.at[ck], br0.at[k, mb, part], partner).start()

        @pl.when(line == 0)
        def _():
            pltpu.make_async_copy(o_v.at[ck, 0, cols], bk_ref.at[k, mb, 0, 0, cols], b0.at[ck]).start()

        for rc in range(1, n_blk):
            r, cc = rc // 2, rc % 2
            back = ((n_x - r) % n_x) * 2 + cc
            remote(o_v.at[ck, rc, cols], bk_ref.at[k, mb, line, back, cols], bs.at[ck], br.at[k, ck, part],
                   dev(line, r, cc)).start()

    def sent_wait(ck):
        many = o_v.at[ck, pl.ds(1, n_blk - 1)]
        pltpu.make_async_copy(many, many, bs.at[ck]).wait()
        one = o_v.at[ck, 0]
        pltpu.make_async_copy(one, one, b0.at[ck]).wait()

    def down(ck, begin, end):
        def tile(n, carry):
            part = n // n_part
            cols = pl.ds(pl.multiple_of((n % n_part) * n_tile, n_tile), n_tile)
            out = jnp.dot(h_v[ck], wd_v[part, :, cols], preferred_element_type=jnp.float32).astype(jnp.bfloat16)
            o_v[ck, :, part, :, cols] = out.reshape(n_blk, cap, n_tile)
            return carry

        lax.fori_loop(begin * n_part, end * n_part, tile, 0)

    def compute(k):
        row_load(k, 0).start()
        for a in range(3):
            w_load(3, k, a).start()
        for a in range(3):
            w_load(1, k, a).start()
        for a in range(3):
            w_copy(0, k, a).wait_recv()
            w_load(0, k, a).start()
        for a in range(2):
            w_copy(2, k, a).wait_recv()
            w_load(2, k, a).start()
        for j in range(4):
            for a in range(2):
                w_load(j, k, a).wait()

        def up_chunk(ck, carry):
            slot = ck % 2
            row_load(k, ck).wait()

            @pl.when(ck + 1 < n_chunk)
            def _():
                row_load(k, ck + 1).start()

            def up_tile(f, carry):
                cols = pl.ds(pl.multiple_of(f * LANES, LANES), LANES)
                both = jnp.concatenate([wg_v[:, cols], wu_v[:, cols]], axis=1)
                pre = jnp.dot(rows_v[slot].reshape(rows_chunk, d_model), both, preferred_element_type=jnp.float32)
                h_v[ck, :, cols] = (jax.nn.silu(pre[:, :LANES]) * pre[:, LANES:]).astype(jnp.bfloat16)
                return carry

            lax.fori_loop(0, ff // LANES, up_tile, 0)

            @pl.when(k > 0)
            def _():
                sent_wait(ck)

            down(ck, 0, 3)
            send(k, ck, 0)
            return carry

        for j in (3, 0, 1):
            w_load(j, k, 2).wait()
        lax.fori_loop(0, n_chunk, up_chunk, 0)
        w_copy(2, k, 2).wait_recv()
        w_load(2, k, 2).start()
        w_load(2, k, 2).wait()

        def down_chunk(ck, carry):
            down(ck, 3, 4)
            send(k, ck, 1)
            return carry

        lax.fori_loop(0, n_chunk, down_chunk, 0)

    n_grp = n_blk // 4
    k_rows = 4 * cap

    n_unit = 2 * n_chunk * n_grp

    def mix_of(u):
        v = u // n_grp
        return v // n_chunk, v // n_mb % 2, v % n_mb

    def o_load(k, u, part):
        _, line, mb = mix_of(u)
        cols = parts[part]
        return pltpu.make_async_copy(bk_ref.at[k, mb, line, pl.ds((u % n_grp) * 4, 4), cols],
                                     ob_v.at[u % 2, pl.ds(0, 4), cols], osem.at[u % 2])

    def o_ready(k, u):
        now, line, mb = mix_of(u)
        ck = (1 - line) * n_mb + mb
        for part in range(2):
            @pl.when(jnp.logical_and(u % n_grp == 0, now == part))
            def _():
                many = bk_ref.at[k, mb, line, pl.ds(1, n_blk - 1), parts[part]]
                pltpu.make_async_copy(many, many, br.at[k, ck, part]).wait()

                @pl.when(line == 1)
                def _():
                    one = bk_ref.at[k, mb, line, 0, parts[part]]
                    pltpu.make_async_copy(one, one, br0.at[k, mb, part]).wait()

            @pl.when(now == part)
            def _():
                o_load(k, u, part).start()

    def combine(k):
        o_ready(k, 0)

        def unit(u, carry):
            now, line, mb = mix_of(u)
            slot = u % 2
            mixes = []
            for i in range(4):
                q = quad(line, (u % n_grp) * 4 + i)
                hit = p_v[q, pl.ds(mb * half + k, 1), :] == place_i
                mixes.append(jnp.where(hit, g_v[q, pl.ds(mb * half + k, 1), :], 0.0))
            mix = jnp.concatenate(mixes, axis=0).T
            first = mix.astype(jnp.bfloat16)
            rest = mix - first.astype(jnp.float32)
            second = rest.astype(jnp.bfloat16)
            third = (rest - second.astype(jnp.float32)).astype(jnp.bfloat16)
            lt_v[:, 0:k_rows] = first
            lt_v[:, k_rows:2 * k_rows] = second
            lt_v[:, 2 * k_rows:3 * k_rows] = third
            for part in range(2):
                @pl.when(now == part)
                def _():
                    o_load(k, u, part).wait()

            @pl.when((u + 1) % n_grp != 0)
            def _():
                o_ready(k, u + 1)

            d_src = d + line * (3 - 2 * d)

            def tile(n, carry):
                part = n // n_part
                owner = d_src + (part % 2) * (1 - 2 * (d_src % 2))
                owner = owner + (part // 2) * (3 - 2 * owner)
                cols = pl.ds(pl.multiple_of((n % n_part) * n_tile, n_tile), n_tile)
                rows = ob_v[slot, :, part, :, cols].reshape(k_rows, n_tile)
                at = pl.ds(pl.multiple_of(owner * d_loc + (n % n_part) * n_tile, n_tile), n_tile)
                acc_v[mb, :, at] += jnp.dot(lt_v[...], jnp.concatenate([rows, rows, rows], axis=0),
                                              preferred_element_type=jnp.float32)
                return carry

            lax.fori_loop(now * 3 * n_part, (3 + now) * n_part, tile, 0)

            @pl.when(jnp.logical_and((u + 1) % n_grp == 0, u + 1 < n_unit))
            def _():
                o_ready(k, u + 1)

            @pl.when(jnp.logical_and(k == half - 1, u + 1 >= n_unit - (n_mb - 1 - mb) * n_grp))
            def _():
                rows_v[mb] = acc_v[mb].astype(jnp.bfloat16).reshape(n_blk, cap, d_model)
                pltpu.make_async_copy(rows_v.at[mb], y_ref.at[mb], ysem.at[mb]).start()

            return carry

        lax.fori_loop(0, n_unit, unit, 0)

    def step(k, carry):
        @pl.when(k < half)
        def _():
            compute(k)

        @pl.when(k + 2 < half)
        def _():
            w_forward(k + 2)

        @pl.when(k == 0)
        def _():
            w_start(0, half - 1)

        @pl.when(k == half)
        def _():
            for ck in range(n_chunk):
                sent_wait(ck)

        @pl.when(k > 0)
        def _():
            combine(k - 1)

        return carry

    lax.fori_loop(0, half + 1, step, 0)

    for flow in range(3):
        for k in range(half):
            for a in range(3):
                w_copy(flow, k, a).wait_send()
    for line in range(2):
        for mb in range(n_mb):
            for r in range(n_x):
                for cc in range(2):
                    if (line, r, cc) != (0, 0, 0):
                        x_copy(line, mb, r, cc).wait_send()
    for line in range(2):
        for r in range(n_x):
            for cc in range(2):
                if (line, r, cc) != (0, 0, 0):
                    p_copy(line, r, cc).wait_send()
    for mb in range(n_mb):
        pltpu.make_async_copy(rows_v.at[mb], y_ref.at[mb], ysem.at[mb]).wait()


def solution(mesh):
    expert_devs = mesh.shape['expert']
    n_x = expert_devs // 2
    row_spec = P(None, ('rep', 'expert', 'data'), None)
    up_spec = P('expert', 'data', None)
    down_spec = P('expert', None, 'data')

    def per_device(x_loc, idx_loc, gate_loc, wg_loc, wu_loc, wd_loc):
        n_mb, tok, d_model = x_loc.shape
        n_top = idx_loc.shape[2]
        n_loc, d_loc, ff = wg_loc.shape
        n_exp = n_loc * expert_devs
        half = n_loc // 2
        cap = 8 * ((5 * n_top * tok + 32 * n_exp - 1) // (32 * n_exp))
        assert tok == expert_devs * cap
        bf16, f32 = jnp.bfloat16, jnp.float32
        n_quad = 2 * expert_devs
        rows = (expert_devs, cap, d_model)
        shards = (expert_devs, 4, cap, d_loc)
        hbm = pl.BlockSpec(memory_space=pl.ANY)
        vmem = pl.BlockSpec(memory_space=pltpu.VMEM)
        dma = pltpu.SemaphoreType.DMA
        out = pl.pallas_call(
            functools.partial(moe_kernel, n_x, cap),
            out_shape=[
                jax.ShapeDtypeStruct((n_mb,) + rows, bf16),
                jax.ShapeDtypeStruct((n_mb, n_quad) + rows, bf16),
                jax.ShapeDtypeStruct((half, n_mb, 2) + rows, bf16),
                jax.ShapeDtypeStruct((half, n_mb, 2) + shards, bf16),
                jax.ShapeDtypeStruct((3, half, d_loc, ff), bf16),
                jax.ShapeDtypeStruct((3, half, d_loc, ff), bf16),
                jax.ShapeDtypeStruct((3, half, ff, d_loc), bf16),
            ],
            in_specs=[hbm, vmem, vmem, hbm, hbm, hbm],
            out_specs=[hbm] * 7,
            scratch_shapes=[
                pltpu.VMEM((4 * d_loc, ff), bf16),
                pltpu.VMEM((4 * d_loc, ff), bf16),
                pltpu.VMEM((4, ff, d_loc), bf16),
                pltpu.VMEM((2,) + rows, bf16),
                pltpu.VMEM((2 * n_mb,) + shards, bf16),
                pltpu.VMEM((2 * n_mb, tok, ff), bf16),
                pltpu.VMEM((n_mb, tok, d_model), f32),
                pltpu.VMEM((2, half, cap, d_model), bf16),
                pltpu.VMEM((2, 4, 4, cap, d_loc), bf16),
                pltpu.VMEM((tok, 12 * cap), bf16),
                pltpu.VMEM((n_quad, n_mb * half, tok), f32),
                pltpu.VMEM((n_quad, n_mb * half, tok), f32),
                pltpu.VMEM((n_quad, n_mb * half, tok), f32),
                dma((3, half, 3)), dma((3, half, 3)), dma((4, 3)),
                dma((n_mb, n_quad)), dma((n_mb, n_quad)),
                dma((n_quad,)), dma((n_quad,)),
                dma((2,)), dma((2,)), dma((2,)),
                dma((2 * n_mb,)), dma((2 * n_mb,)),
                dma((half, 2 * n_mb, 2)), dma((half, n_mb, 2)),
                dma((2,)), dma((2,)),
            ],
            compiler_params=pltpu.CompilerParams(collective_id=0, has_side_effects=True, vmem_limit_bytes=62 * 1024 * 1024),
        )(x_loc.reshape((n_mb,) + rows), idx_loc.transpose(2, 0, 1), gate_loc.transpose(2, 0, 1), wg_loc, wu_loc, wd_loc)
        return out[0].reshape(n_mb, tok, d_model)

    return jax.shard_map(per_device, mesh=mesh, in_specs=(row_spec, row_spec, row_spec, up_spec, up_spec, down_spec),
                         out_specs=row_spec, check_vma=False)
```
